32 devices in a mesh: dp: 8 (over z, core), tensor: 4 (over y, x).
Axes of the slice: x: 2, y: 2, z: 4, core: 2. Of those that a mesh axis runs over, the one named last changes fastest.
Arguments:
- queries: bfloat16 [3584, 8192], P('dp', 'tensor'), may hold values from -6 to 6
- features: bfloat16 [16, 384, 8192], P('dp', None, 'tensor'), may hold values from -6 to 6
- kv_weight: bfloat16 [8192, 2048], P('tensor'), may hold values from -0.0625 to 0.0625
- q_gain: float32 [128], replicated, may hold values from 0.5 to 2
- k_gain: float32 [128], replicated, may hold values from 0.5 to 2
- counts: int32 [16], replicated, may hold values from 1 to 16, as said below
- owner: int32 [16], replicated, may hold values from 0 to 15, as said below
Outputs:
- attended: bfloat16 [3584, 8192], P('dp', 'tensor')
The draws below stay inside these ranges and needn't reach their ends.
Inputs may be any that keep to these rules, and one draw needn't show every extreme that they name: `counts`: every sample has 1 to 16 images; in every draw some sample has 16 and some has one. `owner`: there are 2 different shifts c_j, each from 0 to the number of dp indices minus 1; sample s = e * 2 + j goes to slot ((e + c_j) modulo the number of dp indices) * 2 + j, with the same c_j for every e.
All inputs are finite; a program needn't handle non-finite values.
Results may differ from the reference program's by a relative error of at most 0.028.
Values may be sent and summed in bfloat16 or wider, within the bound.
No kernel may reach another device: no remote copies, remote signals or barrier semaphores. Data moves between devices by JAX's collectives and lax.ppermute only.
A program may use at most 64 MiB of HBM per device.

```python
import math
import jax
import jax.numpy as jnp
from jax import lax

VIS = 8192
QH = 64
KVH = 8
HD = 128
TXT = 224
PATCH = 24
MAX_IMAGES = 16
SAMP_DEV = 2
SAMPLES = 16
N_TENSOR = 4


def draw_counts(key, part):
    first_key, second_key = jax.random.split(jax.random.fold_in(key, 11), 2)
    drawn = jax.random.randint(first_key, (SAMPLES,), 1, MAX_IMAGES + 1).astype(jnp.int32)
    chosen = jax.random.permutation(second_key, SAMPLES)[:2]
    drawn = drawn.at[chosen[0]].set(MAX_IMAGES)
    drawn = drawn.at[chosen[1]].set(1)
    return drawn.astype(jnp.int32)


def draw_owner(key, part):
    shard_total = SAMPLES // SAMP_DEV
    base_key = jax.random.fold_in(key, 23)
    shift_list = jax.random.permutation(base_key, shard_total).astype(jnp.int32)[:SAMP_DEV]
    encoder = jnp.arange(shard_total, dtype=jnp.int32)[:, None]
    position = jnp.arange(SAMP_DEV, dtype=jnp.int32)[None, :]
    target = (encoder + shift_list[None, :]) % shard_total
    return (target * SAMP_DEV + position).reshape(-1).astype(jnp.int32)


def shard_levels(own_key, extent, cuts, low, largest):
    factor_of = 1.0
    for dim, blocks in cuts:
        draws = jax.random.uniform(jax.random.fold_in(jax.random.fold_in(own_key, 6), dim), (blocks,), jnp.float32, low / len(cuts), largest / len(cuts))
        factor_of = factor_of * jnp.repeat(jnp.exp(draws), extent[dim] // blocks).reshape((-1,) + (1,) * (len(extent) - 1 - dim))
    return factor_of


def scatter_about(own_key, dims, deviation, most, shards=(), kind=jnp.bfloat16):
    result = deviation * jax.random.normal(own_key, dims, jnp.float32)
    if shards:
        result = result * shard_levels(own_key, dims, shards, -0.22, 0.18)
    return jnp.clip(result, -most, most).astype(kind)


def setup_inputs(seed: int = 0) -> dict:
    arg_keys = jax.random.split(jax.random.key(seed), 8)
    queries = scatter_about(arg_keys[0], (SAMPLES * TXT, QH * HD), 1.0, 6.0, ((0, 8), (1, 4)))
    features = scatter_about(arg_keys[1], (SAMPLES, MAX_IMAGES * PATCH, VIS), 1.0, 6.0, ((0, 8), (2, 4)))
    kv_weight = scatter_about(arg_keys[2], (VIS, 2 * KVH * HD), VIS ** -0.5, 0.0625, ((0, 4),))
    q_gain = jnp.clip(jnp.exp(jax.random.uniform(arg_keys[3], (HD,), jnp.float32, math.log(0.5), math.log(2.0))), 0.5, 2.0)
    k_gain = jnp.clip(jnp.exp(jax.random.uniform(arg_keys[4], (HD,), jnp.float32, math.log(0.5), math.log(2.0))), 0.5, 2.0)
    counts = draw_counts(jax.random.fold_in(arg_keys[7], 71), 0)
    owner = draw_owner(jax.random.fold_in(arg_keys[7], 71), 0)
    return {"queries": queries, "features": features, "kv_weight": kv_weight, "q_gain": q_gain, "k_gain": k_gain, "counts": counts, "owner": owner}


def normalize_rows(values_in, gain):
    return values_in * lax.rsqrt(lax.optimization_barrier(jnp.mean(values_in * values_in, axis=-1, keepdims=True)) + 1e-05) * gain

def reference(queries, features, kv_weight, q_gain, k_gain, counts, owner):
    group_size = QH // KVH
    token_count = features.shape[1]
    piece_width = VIS // N_TENSOR
    weight_groups = kv_weight.astype(jnp.float32).reshape(N_TENSOR, piece_width, 2 * KVH * HD)
    source_of = jnp.zeros((SAMPLES,), jnp.int32).at[owner].set(jnp.arange(SAMPLES, dtype=jnp.int32))
    query_blocks = queries.reshape(SAMPLES, TXT, QH, HD)

    def attend_slot(slot_id):
        sample = source_of[slot_id]
        feature_rows = features[sample].astype(jnp.float32).reshape(token_count, N_TENSOR, piece_width)
        partials = jnp.einsum('rnc,ncf->nrf', feature_rows, weight_groups)
        partials = lax.optimization_barrier(partials.astype(jnp.bfloat16)).astype(jnp.float32)
        projected = lax.optimization_barrier(jnp.sum(partials, axis=0)).reshape(token_count, KVH, 2, HD)
        key_heads = normalize_rows(projected[:, :, 0], k_gain).astype(jnp.bfloat16)
        value_heads = projected[:, :, 1].astype(jnp.bfloat16)
        query_here = normalize_rows(query_blocks[slot_id].astype(jnp.float32), q_gain) / math.sqrt(HD)
        query_here = lax.optimization_barrier(query_here.astype(jnp.bfloat16)).astype(jnp.float32)
        key_here = jnp.repeat(key_heads, group_size, axis=1).astype(jnp.float32)
        value_here = jnp.repeat(value_heads, group_size, axis=1).astype(jnp.float32)
        scores = jnp.einsum('tqd,rqd->qtr', query_here, key_here)
        valid_keys = jnp.arange(token_count, dtype=jnp.int32) < counts[sample] * PATCH
        exponent = jnp.where(valid_keys[None, None, :], jnp.exp(scores), 0.0)
        weights = (exponent / lax.optimization_barrier(jnp.sum(exponent, axis=-1, keepdims=True))).astype(jnp.bfloat16)
        weights = lax.optimization_barrier(weights).astype(jnp.float32)
        context = jnp.einsum('qtr,rqd->tqd', weights, value_here)
        return context.astype(jnp.bfloat16).reshape(TXT, QH * HD)
    attended = lax.map(attend_slot, jnp.arange(SAMPLES, dtype=jnp.int32))
    return attended.reshape(SAMPLES * TXT, QH * HD)
```

```python
import functools
import math

import jax
import jax.numpy as jnp
from jax import lax
from jax.experimental import pallas as pl
from jax.experimental.pallas import tpu as pltpu
from jax.sharding import PartitionSpec as P

HD = 128
PATCH = 24
EPS = 1e-05
DIGIT = 8


def project_body(first_block, place_ref, feature_ref, weight_ref, *out_refs):
    block = pl.program_id(0)
    part = pl.program_id(1)
    width = weight_ref.shape[1]
    partial = jnp.dot(
        feature_ref[0], weight_ref[...], preferred_element_type=jnp.float32
    ).astype(jnp.bfloat16)
    columns = pl.ds(pl.multiple_of(part * width, width), width)
    for k, out_ref in enumerate(out_refs):
        @pl.when(block == k)
        def _():
            out_ref[:, columns] = partial


def project(place, features, kv_weight, first_block, block_count, head_cols, repeats):
    _, token_count, depth = features.shape
    width = min(head_cols, 256)
    parts = head_cols // width

    def weight_index(block, part, place_ref):
        other = jnp.bitwise_xor(place_ref[1], block + first_block)
        return 0, lax.div(other, jnp.int32(repeats)) * parts + part

    shape = jax.ShapeDtypeStruct((token_count, head_cols), jnp.bfloat16)
    return pl.pallas_call(
        functools.partial(project_body, first_block),
        grid_spec=pltpu.PrefetchScalarGridSpec(
            num_scalar_prefetch=1,
            grid=(block_count, parts),
            in_specs=[
                pl.BlockSpec((1, token_count, depth), lambda b, p, place_ref: (place_ref[0], 0, 0)),
                pl.BlockSpec((depth, width), weight_index),
            ],
            out_specs=[
                pl.BlockSpec((token_count, head_cols), lambda b, p, place_ref: (0, 0))
            ] * block_count,
        ),
        out_shape=[shape] * block_count,
        cost_estimate=pl.CostEstimate(
            flops=2 * token_count * depth * head_cols * block_count,
            bytes_accessed=2 * (token_count * depth + depth * head_cols * block_count),
            transcendentals=0,
        ),
        compiler_params=pltpu.CompilerParams(
            dimension_semantics=("arbitrary", "arbitrary"), vmem_limit_bytes=60 << 20
        ),
        name="project",
    )(place, features, kv_weight)


def combine_body(gain_ref, *refs):
    part_refs, out_ref = refs[:-1], refs[-1]
    total = part_refs[0][...].astype(jnp.float32)
    for ref in part_refs[1:]:
        total = total + ref[...].astype(jnp.float32)
    for column in range(0, out_ref.shape[1], 2 * HD):
        key = total[:, column : column + HD]
        scale = lax.rsqrt(jnp.mean(key * key, axis=-1, keepdims=True) + EPS)
        out_ref[:, column : column + HD] = (key * scale * gain_ref[...]).astype(jnp.bfloat16)
        out_ref[:, column + HD : column + 2 * HD] = total[
            :, column + HD : column + 2 * HD
        ].astype(jnp.bfloat16)


def combine(k_gain, parts):
    rows, cols = parts[0].shape
    tile = rows // 4
    block = pl.BlockSpec((tile, cols), lambda i: (i, 0))
    return pl.pallas_call(
        combine_body,
        grid=(rows // tile,),
        in_specs=[pl.BlockSpec((1, HD), lambda i: (0, 0))] + [block] * len(parts),
        out_specs=block,
        out_shape=jax.ShapeDtypeStruct((rows, cols), jnp.bfloat16),
        cost_estimate=pl.CostEstimate(
            flops=rows * cols * (len(parts) + 4),
            bytes_accessed=2 * rows * cols * (len(parts) + 1),
            transcendentals=rows,
        ),
        compiler_params=pltpu.CompilerParams(vmem_limit_bytes=60 << 20),
        name="combine",
    )(k_gain, *parts)


def query_norm_body(gain_ref, query_ref, out_ref):
    for column in range(0, query_ref.shape[1], HD):
        head = query_ref[:, column : column + HD].astype(jnp.float32)
        scale = lax.rsqrt(jnp.mean(head * head, axis=-1, keepdims=True) + EPS)
        out_ref[:, column : column + HD] = (
            head * scale * gain_ref[...] * (1.0 / math.sqrt(HD))
        ).astype(jnp.bfloat16)


def query_norm(q_gain, queries):
    rows, cols = queries.shape
    tile = rows // 4
    block = pl.BlockSpec((tile, cols), lambda i: (i, 0))
    return pl.pallas_call(
        query_norm_body,
        grid=(rows // tile,),
        in_specs=[pl.BlockSpec((1, HD), lambda i: (0, 0)), block],
        out_specs=block,
        out_shape=jax.ShapeDtypeStruct((rows, cols), jnp.bfloat16),
        cost_estimate=pl.CostEstimate(
            flops=rows * cols * 6, bytes_accessed=4 * rows * cols, transcendentals=rows * cols // HD
        ),
        compiler_params=pltpu.CompilerParams(vmem_limit_bytes=60 << 20),
        name="query_norm",
    )(q_gain, queries)


def attend_body(group, has_base, place_ref, query_ref, kv_ref, *refs):
    out_ref = refs[-1]
    token_count = kv_ref.shape[0]
    rows = lax.broadcasted_iota(jnp.int32, (token_count, HD), 0)
    keep = rows < place_ref[1] * PATCH
    zero = jnp.zeros((token_count, HD), jnp.float32)
    ones = jnp.where(keep, zero + 1.0, zero).astype(jnp.bfloat16)
    for start in range(0, query_ref.shape[1], group * HD):
        column = start // group * 2
        key = kv_ref[:, column : column + HD]
        value = jnp.where(
            keep, kv_ref[:, column + HD : column + 2 * HD].astype(jnp.float32), zero
        ).astype(jnp.bfloat16)
        value_ones = jnp.concatenate([value, ones], axis=1)
        for lane in range(start, start + group * HD, HD):
            scores = lax.dot_general(
                query_ref[:, lane : lane + HD],
                key,
                (((1,), (1,)), ((), ())),
                preferred_element_type=jnp.float32,
            )
            exponent = jnp.exp(scores).astype(jnp.bfloat16)
            summed = jnp.dot(exponent, value_ones, preferred_element_type=jnp.float32)
            out_ref[:, lane : lane + HD] = (summed[:, :HD] / summed[:, HD:]).astype(jnp.bfloat16)


def attend(place, query_normed, kv, base, group, text_len):
    rows, cols = query_normed.shape
    token_count, kv_cols = kv.shape
    kv_heads = kv_cols // (2 * HD)
    width = group * HD
    in_specs = [
        pl.BlockSpec((text_len, width), lambda h, place_ref: (place_ref[0], h)),
        pl.BlockSpec((token_count, 2 * HD), lambda h, place_ref: (0, h)),
    ]
    operands = [place, query_normed, kv]
    aliases = {}
    if base is not None:
        in_specs.append(pl.BlockSpec(memory_space=pl.ANY))
        operands.append(base)
        aliases = {3: 0}
    heads = cols // HD
    return pl.pallas_call(
        functools.partial(attend_body, group, base is not None),
        grid_spec=pltpu.PrefetchScalarGridSpec(
            num_scalar_prefetch=1,
            grid=(kv_heads,),
            in_specs=in_specs,
            out_specs=pl.BlockSpec((text_len, width), lambda h, place_ref: (place_ref[0], h)),
        ),
        out_shape=jax.ShapeDtypeStruct((rows, cols), jnp.bfloat16),
        input_output_aliases=aliases,
        cost_estimate=pl.CostEstimate(
            flops=6 * heads * text_len * token_count * HD,
            bytes_accessed=4 * text_len * cols + 2 * token_count * kv_cols,
            transcendentals=heads * text_len * token_count,
        ),
        compiler_params=pltpu.CompilerParams(vmem_limit_bytes=60 << 20),
        name="attend",
    )(*operands)


def shifted(value, by):
    length = lax.axis_size("dp")
    if by % length == 0:
        return value
    return lax.ppermute(value, "dp", [(i, (i + by) % length) for i in range(length)])


def routed(value, shift):
    length = lax.axis_size("dp")
    unit = 1
    while unit < length:
        choices = min(DIGIT, -(-length // unit))
        value = lax.switch(
            lax.rem(lax.div(shift, jnp.int32(unit)), jnp.int32(choices)),
            [functools.partial(shifted, by=unit * k) for k in range(choices)],
            value,
        )
        unit *= choices
    return value


def shards(queries, features, kv_weight, q_gain, k_gain, counts, owner):
    samples_here = features.shape[0]
    dp_count = lax.axis_size("dp")
    tensor_count = lax.axis_size("tensor")
    dp_index = lax.axis_index("dp").astype(jnp.int32)
    tensor_index = lax.axis_index("tensor").astype(jnp.int32)
    local_width = kv_weight.shape[1] // tensor_count
    repeats = max(1, 2 * HD // local_width)
    head_cols = local_width * repeats
    kv_heads = head_cols // (2 * HD)
    group = queries.shape[1] // HD // kv_heads
    text_len = queries.shape[0] // samples_here

    shifts = owner[:samples_here] // samples_here
    reach = jnp.minimum(shifts, dp_count - shifts)
    slots = [jnp.int32(j) for j in range(samples_here)]
    if samples_here == 2:
        swap = (reach[1] > reach[0]).astype(jnp.int32)
        slots = [swap, 1 - swap]

    k_gain = k_gain.reshape(1, HD)
    q_gain = q_gain.reshape(1, HD)
    arrived = []
    for slot in slots:
        place = jnp.stack([slot, tensor_index])
        sent = project(place, features, kv_weight, 1, tensor_count - 1, head_cols, repeats)
        arrived.append(
            [
                lax.ppermute(part, "tensor", [(i, i ^ (j + 1)) for i in range(tensor_count)])
                for j, part in enumerate(sent)
            ]
        )
    own = [
        project(jnp.stack([slot, tensor_index]), features, kv_weight, 0, 1, head_cols, repeats)[0]
        for slot in slots
    ]
    query_normed = query_norm(q_gain, queries)
    out = None
    for k, slot in enumerate(slots):
        shift = shifts[slot]
        source = lax.rem(dp_index - shift + dp_count, dp_count) * samples_here + slot
        kv = combine(k_gain, [own[k]] + arrived[k])
        kv = routed(kv, shift)
        out = attend(
            jnp.stack([slot, counts[source]]), query_normed, kv, out, group, text_len
        )
    return out


def solution(mesh):
    placed = (P("dp", "tensor"), P("dp", None, "tensor"), P("tensor", None), P(), P(), P(), P())
    return jax.shard_map(
        shards, mesh=mesh, in_specs=placed, out_specs=P("dp", "tensor"), check_vma=False
    )
```

```python
import functools
import math

import jax
import jax.numpy as jnp
from jax import lax
from jax._src.lax.control_flow import conditionals
from jax.experimental import pallas as pl
from jax.experimental.pallas import tpu as pltpu
from jax.sharding import PartitionSpec as P

HD = 128
PATCH = 24
EPS = 1e-05
DIGIT = 8


def ranked_slot(rank, owner_ref, samples_here, dp_count):
    if samples_here != 2:
        return rank
    reach = []
    for j in range(2):
        shift = lax.div(owner_ref[j], jnp.int32(2))
        reach.append(jnp.minimum(shift, dp_count - shift))
    return jnp.where(reach[1] > reach[0], 1 - rank, rank)


def project_body(samples_here, dp_count, repeats, wanted, head_cols, owner_ref, feature_hbm, weight_hbm, *rest):
    out_refs = rest[: len(wanted)]
    features, weights, feature_sem, weight_sem = rest[len(wanted) :]
    me = lax.axis_index("tensor").astype(jnp.int32)
    ranks = list(dict.fromkeys(rank for rank, _, _, _ in wanted))
    blocks = list(dict.fromkeys(block for _, _, _, blocks in wanted for block in blocks))
    pieces, depth = weights.shape[1], weights.shape[2]

    def feature_copy(rank, piece):
        slot = ranked_slot(rank, owner_ref, samples_here, dp_count)
        k = ranks.index(rank)
        return pltpu.make_async_copy(
            feature_hbm.at[slot, :, pl.ds(piece * depth, depth)],
            features.at[k, piece],
            feature_sem.at[k, piece],
        )

    def weight_copy(block, piece):
        head = lax.div(jnp.bitwise_xor(me, block), jnp.int32(repeats))
        start = pl.multiple_of(head * head_cols, 2 * HD)
        k = blocks.index(block)
        return pltpu.make_async_copy(
            weight_hbm.at[pl.ds(piece * depth, depth), pl.ds(start, head_cols)],
            weights.at[k, piece],
            weight_sem.at[k, piece],
        )

    jobs = [
        (out_ref, rank, row, count, k, block)
        for out_ref, (rank, row, count, row_blocks) in zip(out_refs, wanted)
        for k, block in enumerate(row_blocks)
    ]
    jobs.sort(key=lambda job: (ranks.index(job[1]), blocks.index(job[5])))
    copies = {}
    for _, rank, _, _, _, block in jobs:
        for piece in range(pieces):
            for kind, name in (("f", rank), ("w", block)):
                if (kind, name, piece) not in copies:
                    copy = (feature_copy if kind == "f" else weight_copy)(name, piece)
                    copies[kind, name, piece] = copy
                    copy.start()
    waited = set()
    for out_ref, rank, row, count, k, block in jobs:
        total = None
        for piece in range(pieces):
            for entry in (("f", rank, piece), ("w", block, piece)):
                if entry not in waited:
                    copies[entry].wait()
                    waited.add(entry)
            term = jnp.dot(
                features[ranks.index(rank), piece, row : row + count],
                weights[blocks.index(block), piece],
                preferred_element_type=jnp.float32,
            )
            total = term if total is None else total + term
        out_ref[:, k * head_cols : (k + 1) * head_cols] = total.astype(jnp.bfloat16)


def project(owner, features, kv_weight, wanted, pieces, head_cols, repeats):
    samples_here, token_count, depth = features.shape
    ranks = len({rank for rank, _, _, _ in wanted})
    blocks = len({block for _, _, _, blocks in wanted for block in blocks})
    work = sum(count * len(row_blocks) for _, _, count, row_blocks in wanted)
    hbm = pl.BlockSpec(memory_space=pltpu.HBM)
    return pl.pallas_call(
        functools.partial(
            project_body, samples_here, lax.axis_size("dp"), repeats, wanted, head_cols
        ),
        in_specs=[pl.BlockSpec(memory_space=pltpu.SMEM), hbm, hbm],
        out_specs=[pl.BlockSpec(memory_space=pltpu.VMEM)] * len(wanted),
        out_shape=[
            jax.ShapeDtypeStruct((count, head_cols * len(row_blocks)), jnp.bfloat16)
            for _, _, count, row_blocks in wanted
        ],
        scratch_shapes=[
            pltpu.VMEM((ranks, pieces, token_count, depth // pieces), jnp.bfloat16),
            pltpu.VMEM((blocks, pieces, depth // pieces, head_cols), jnp.bfloat16),
            pltpu.SemaphoreType.DMA((ranks, pieces)),
            pltpu.SemaphoreType.DMA((blocks, pieces)),
        ],
        cost_estimate=pl.CostEstimate(
            flops=2 * work * depth * head_cols,
            bytes_accessed=2 * (token_count * ranks + head_cols * blocks) * depth,
            transcendentals=0,
        ),
        compiler_params=pltpu.CompilerParams(vmem_limit_bytes=58 << 20),
        name="project",
    )(owner, features, kv_weight)


def mean_square(value):
    square = value * value
    high = square.astype(jnp.bfloat16)
    low = (square - high.astype(jnp.float32)).astype(jnp.bfloat16)
    parts = jnp.concatenate([high, low], axis=1)
    ones = jnp.ones((2 * HD, HD), jnp.bfloat16)
    return jnp.dot(parts, ones, preferred_element_type=jnp.float32) * (1.0 / HD)


def add_body(*refs):
    count = len(refs) // 3
    for k in range(count):
        ref, other, out_ref = refs[2 * k], refs[2 * k + 1], refs[2 * count + k]
        cols = out_ref.shape[1]
        out_ref[...] = (
            ref[:, cols:].astype(jnp.float32) + other[:, cols:].astype(jnp.float32)
        ).astype(jnp.bfloat16)


def add_halves(pairs):
    vmem = pl.BlockSpec(memory_space=pltpu.VMEM)
    shapes = [jax.ShapeDtypeStruct((p.shape[0], p.shape[1] // 2), p.dtype) for p, _ in pairs]
    return pl.pallas_call(
        add_body,
        in_specs=[vmem] * (2 * len(pairs)),
        out_specs=[vmem] * len(pairs),
        out_shape=shapes,
        cost_estimate=pl.CostEstimate(
            flops=sum(shape.size for shape in shapes),
            bytes_accessed=6 * sum(shape.size for shape in shapes),
            transcendentals=0,
        ),
        compiler_params=pltpu.CompilerParams(vmem_limit_bytes=16 << 20),
        name="add_halves",
    )(*[part for pair in pairs for part in pair])


def combine_body(layout, gain_ref, *refs):
    out_ref = refs[-1]
    cols = out_ref.shape[1]
    gain = gain_ref[...]
    row = 0
    at = 0
    for count in layout:
        part_refs = refs[at : at + count]
        at += count
        rows = part_refs[0].shape[0]
        for column in range(0, cols, HD):
            lanes = slice(column, column + HD)
            total = part_refs[0][:, lanes].astype(jnp.float32)
            for ref in part_refs[1:]:
                total = total + ref[:, lanes].astype(jnp.float32)
            if column % (2 * HD) == 0:
                total = total * lax.rsqrt(mean_square(total) + EPS) * gain
            out_ref[row : row + rows, lanes] = total.astype(jnp.bfloat16)
        row += rows


def combine(k_gain, groups, head_cols):
    rows = sum(group[0].shape[0] for group in groups)
    parts = sum(len(group) for group in groups)
    vmem = pl.BlockSpec(memory_space=pltpu.VMEM)
    return pl.pallas_call(
        functools.partial(combine_body, [len(group) for group in groups]),
        in_specs=[vmem] * (parts + 1),
        out_specs=vmem,
        out_shape=jax.ShapeDtypeStruct((rows, head_cols), jnp.bfloat16),
        cost_estimate=pl.CostEstimate(
            flops=rows * head_cols * (parts // len(groups) + 4),
            bytes_accessed=2 * rows * head_cols * (parts // len(groups) + 1),
            transcendentals=rows,
        ),
        compiler_params=pltpu.CompilerParams(vmem_limit_bytes=16 << 20),
        name="combine",
    )(k_gain, *[part for group in groups for part in group])


def prepare_body(samples_here, dp_count, owner_ref, gain_ref, query_ref, out_ref, *shift_refs):
    for rank, shift_ref in enumerate(shift_refs):
        slot = ranked_slot(rank, owner_ref, samples_here, dp_count)
        shift_ref[0] = lax.div(owner_ref[slot], jnp.int32(samples_here))
    gain = gain_ref[...] * (1.0 / math.sqrt(HD))
    for column in range(0, query_ref.shape[1], HD):
        head = query_ref[:, column : column + HD].astype(jnp.float32)
        out_ref[:, column : column + HD] = (
            head * lax.rsqrt(mean_square(head) + EPS) * gain
        ).astype(jnp.bfloat16)


def prepare(owner, q_gain, queries, samples_here):
    rows, cols = queries.shape
    tile = cols // 4 if cols % (4 * HD) == 0 else cols
    smem = pl.BlockSpec(memory_space=pltpu.SMEM)
    block = pl.BlockSpec((rows, tile), lambda i: (0, i))
    normed, *shifts = pl.pallas_call(
        functools.partial(prepare_body, samples_here, lax.axis_size("dp")),
        grid=(cols // tile,),
        in_specs=[smem, pl.BlockSpec((1, HD), lambda i: (0, 0)), block],
        out_specs=[block] + [smem] * samples_here,
        out_shape=[jax.ShapeDtypeStruct((rows, cols), jnp.bfloat16)]
        + [jax.ShapeDtypeStruct((1,), jnp.int32)] * samples_here,
        cost_estimate=pl.CostEstimate(
            flops=rows * cols * 6, bytes_accessed=4 * rows * cols, transcendentals=rows * cols // HD
        ),
        compiler_params=pltpu.CompilerParams(vmem_limit_bytes=24 << 20),
        name="prepare",
    )(owner, q_gain, queries)
    return normed, [shift.reshape(()) for shift in shifts]


def attend_body(rank, samples_here, dp_count, group, owner_ref, counts_ref, query_ref, kv_ref, *refs):
    out_ref = refs[-1]
    token_count = kv_ref.shape[0]
    slot = ranked_slot(rank, owner_ref, samples_here, dp_count)
    shift = lax.div(owner_ref[slot], jnp.int32(samples_here))
    source = lax.axis_index("dp").astype(jnp.int32) - shift
    source = jnp.where(source < 0, source + dp_count, source)
    images = counts_ref[source * samples_here + slot]
    rows = lax.broadcasted_iota(jnp.int32, (token_count, HD), 0)
    keep = rows < images * PATCH
    zero = jnp.zeros((token_count, HD), jnp.float32)
    ones = jnp.where(keep, zero + 1.0, zero).astype(jnp.bfloat16)
    key = kv_ref[:, :HD]
    value = jnp.where(keep, kv_ref[:, HD : 2 * HD].astype(jnp.float32), zero).astype(jnp.bfloat16)
    value_ones = jnp.concatenate([value, ones], axis=1)
    text_len = query_ref.shape[0]
    stack = 2 if group % 2 == 0 else 1
    for first in range(0, group, stack):
        lanes = [slice(h * HD, (h + 1) * HD) for h in range(first, first + stack)]
        scores = lax.dot_general(
            jnp.concatenate([query_ref[:, lane] for lane in lanes], axis=0),
            key,
            (((1,), (1,)), ((), ())),
            preferred_element_type=jnp.float32,
        )
        exponent = jnp.exp(scores).astype(jnp.bfloat16)
        summed = jnp.dot(exponent, value_ones, preferred_element_type=jnp.float32)
        context = (summed[:, :HD] / summed[:, HD:]).astype(jnp.bfloat16)
        for k, lane in enumerate(lanes):
            out_ref[:, lane] = context[k * text_len : (k + 1) * text_len]


def attend(owner, counts, query_normed, kv, base, rank, samples_here, group, text_len):
    rows, cols = query_normed.shape
    token_count, kv_cols = kv.shape
    dp_count = lax.axis_size("dp")
    width = group * HD

    def text_index(h, owner_ref, counts_ref):
        return ranked_slot(rank, owner_ref, samples_here, dp_count), h

    in_specs = [
        pl.BlockSpec((text_len, width), text_index),
        pl.BlockSpec((token_count, 2 * HD), lambda h, owner_ref, counts_ref: (0, h)),
    ]
    operands = [owner, counts, query_normed, kv]
    aliases = {}
    if base is not None:
        in_specs.append(pl.BlockSpec(memory_space=pl.ANY))
        operands.append(base)
        aliases = {4: 0}
    heads = cols // HD
    return pl.pallas_call(
        functools.partial(attend_body, rank, samples_here, dp_count, group),
        grid_spec=pltpu.PrefetchScalarGridSpec(
            num_scalar_prefetch=2,
            grid=(cols // width,),
            in_specs=in_specs,
            out_specs=pl.BlockSpec((text_len, width), text_index),
        ),
        out_shape=jax.ShapeDtypeStruct((rows, cols), jnp.bfloat16),
        input_output_aliases=aliases,
        cost_estimate=pl.CostEstimate(
            flops=6 * heads * text_len * token_count * HD,
            bytes_accessed=4 * text_len * cols + 2 * token_count * kv_cols,
            transcendentals=heads * text_len * token_count,
        ),
        compiler_params=pltpu.CompilerParams(vmem_limit_bytes=60 << 20),
        name="attend",
    )(*operands)


def moved(value, by):
    length = lax.axis_size("dp")
    if by % length == 0:
        return value
    return lax.ppermute(value, "dp", [(i, (i + by) % length) for i in range(length)])


def by_shift(shift, start, finish):
    length = lax.axis_size("dp")
    digits = []
    unit = 1
    while unit < length:
        digits.append((unit, min(DIGIT, -(-length // unit))))
        unit *= digits[-1][1]
    if not digits:
        return finish(start(), lambda value: value)

    def choose(unit, choices, work):
        digit = shift
        if unit > 1:
            digit = lax.div(digit, jnp.int32(unit))
        if unit * choices < length:
            digit = lax.rem(digit, jnp.int32(choices))
        return conditionals._switch_internal(
            digit,
            [functools.partial(work, unit * k) for k in range(choices)],
            (),
            branches_platforms=None,
        )

    state = None
    for unit, choices in digits[:-1]:
        held = state

        def work(by):
            return moved(start() if held is None else held, by)

        state = choose(unit, choices, work)
    held = state

    def work(by):
        return finish(start() if held is None else held, lambda value: moved(value, by))

    return choose(*digits[-1], work)


def shards(queries, features, kv_weight, q_gain, k_gain, counts, owner):
    samples_here, token_count, _ = features.shape
    tensor_count = lax.axis_size("tensor")
    local_width = kv_weight.shape[1] // tensor_count
    repeats = max(1, 2 * HD // local_width)
    head_cols = local_width * repeats
    group = queries.shape[1] // HD // (head_cols // (2 * HD))
    text_len = queries.shape[0] // samples_here
    k_gain = k_gain.reshape(1, HD)
    q_gain = q_gain.reshape(1, HD)
    half = token_count // 2

    def partials(wanted, pieces=1):
        return project(owner, features, kv_weight, wanted, pieces, head_cols, repeats)

    def swapped(part, bits):
        return lax.ppermute(part, "tensor", [(i, i ^ bits) for i in range(tensor_count)])

    def attention(rank, kv, base):
        return attend(
            owner, counts, query_normed, kv, base, rank, samples_here, group, text_len
        )

    ranks = range(samples_here)
    if tensor_count == 4:
        def sent_of(rank):
            return [(rank, 0, half, (1, 3)), (rank, half, half, (2, 3))]

        def kept_of(rank):
            return [(rank, 0, half, (0, 2)), (rank, half, half, (0, 1))]

        sent = {0: partials(sent_of(0))}

        def first(rank):
            return [swapped(part, 1 + k) for k, part in enumerate(sent[rank])]

        def second(rank, got):
            return [
                swapped(part, 2 - k) for k, part in enumerate(add_halves(list(zip(kept[rank], got))))
            ]

        def settled(rank, got, then):
            return combine(k_gain, list(zip(kept[rank], got, then)), head_cols)

        got = first(0)
        wanted = kept_of(0)
        for rank in ranks[1:]:
            wanted += sent_of(rank) + kept_of(rank)
        results = partials(wanted)
        kept = {0: results[:2]}
        for rank in ranks[1:]:
            sent[rank] = results[4 * rank - 2 : 4 * rank]
            kept[rank] = results[4 * rank : 4 * rank + 2]
    else:
        blocks = list(range(tensor_count - 1, -1, -1))
        sent = {r: partials([(r, 0, token_count, (block,)) for block in blocks]) for r in ranks}

        def first(rank):
            return [swapped(part, block) for part, block in zip(sent[rank][:-1], blocks)]

        def second(rank, got):
            return []

        def settled(rank, got, then):
            return combine(k_gain, [[sent[rank][-1]] + got], head_cols)

        got = first(0)

    then = second(0, got)
    query_normed, shifts = prepare(owner, q_gain, queries, samples_here)
    kv = out = ready = None
    for rank in ranks:
        held, base, known = kv, out, ready
        last = rank == samples_here - 1

        def start():
            return settled(0, got, then) if known is None else known

        def finish(value, move):
            following = result = None
            if not last:
                coming = first(rank + 1)
            value = move(value)
            if rank > 0:
                result = attention(rank - 1, held, base)
            if last:
                return attention(rank, value, result)
            following = settled(rank + 1, coming, second(rank + 1, coming))
            return (value, following) + (() if result is None else (result,))

        moving = by_shift(shifts[rank], start, finish)
        if last:
            return moving
        kv, ready = moving[:2]
        out = moving[2] if rank > 0 else None


def solution(mesh):
    placed = (P("dp", "tensor"), P("dp", None, "tensor"), P("tensor", None), P(), P(), P(), P())
    return jax.shard_map(
        shards, mesh=mesh, in_specs=placed, out_specs=P("dp", "tensor"), check_vma=False
    )
```

```python
import functools
import math

import jax
import jax.numpy as jnp
from jax import lax
from jax._src.lax.control_flow import conditionals
from jax.experimental import pallas as pl
from jax.experimental.pallas import tpu as pltpu
from jax.sharding import PartitionSpec as P

HD = 128
PATCH = 24
EPS = 1e-05
DIGIT = 8
ATTEND_KIB = 24 << 10


def ranked_slot(rank, owner_ref, samples_here, dp_count):
    if samples_here != 2:
        return rank
    reach = []
    for j in range(2):
        shift = lax.div(owner_ref[j], jnp.int32(2))
        reach.append(jnp.minimum(shift, dp_count - shift))
    return jnp.where(reach[1] > reach[0], 1 - rank, rank)


def project_body(samples_here, dp_count, repeats, wanted, head_cols, waits, splits, owner_ref, feature_hbm, weight_hbm, *rest):
    rest = rest[waits:]
    out_refs = rest[: len(wanted)]
    features, weights, feature_sem, weight_sem = rest[len(wanted) :]
    me = lax.axis_index("tensor").astype(jnp.int32)
    ranks = list(dict.fromkeys(rank for rank, _ in wanted))
    panels = list(dict.fromkeys(panel for _, row in wanted for panel in row))
    width = weights.shape[2]
    rows = features.shape[1] // splits

    def feature_copy(k, part):
        slot = ranked_slot(ranks[k], owner_ref, samples_here, dp_count)
        at = pl.ds(part * rows, rows)
        return pltpu.make_async_copy(
            feature_hbm.at[slot, at], features.at[k, at], feature_sem.at[k, part]
        )

    def weight_copy(k):
        block, piece = panels[k]
        head = lax.div(jnp.bitwise_xor(me, block), jnp.int32(repeats))
        start = pl.multiple_of(head * head_cols + piece * width, width)
        return pltpu.make_async_copy(
            weight_hbm.at[:, pl.ds(start, width)], weights.at[k], weight_sem.at[k]
        )

    feature_copies = [
        [feature_copy(k, part) for part in range(splits)] for k in range(len(ranks))
    ]
    weight_copies = [weight_copy(k) for k in range(len(panels))]
    for copy in feature_copies[0] + weight_copies[:2]:
        copy.start()
    for copies in feature_copies[1:]:
        for copy in copies:
            copy.start()
    for k, panel in enumerate(panels):
        weight_copies[k].wait()
        if k + 2 < len(panels):
            weight_copies[k + 2].start()
        takers = [
            (out_ref, ranks.index(rank), slice(row.index(panel) * width, (row.index(panel) + 1) * width))
            for out_ref, (rank, row) in zip(out_refs, wanted)
            if panel in row
        ]
        for _, r, _ in takers:
            for copy in feature_copies[r]:
                copy.wait()
            feature_copies[r] = []

        @pl.when(owner_ref[0] >= 0)
        def _(takers=takers, k=k):
            joint = len(takers) > 1 and [r for _, r, _ in takers] == list(range(len(ranks)))
            token_count, depth = features.shape[1:]
            lefts = [features[...].reshape(-1, depth)] if joint else [features[r] for _, r, _ in takers]
            products = [
                jnp.dot(left, weights[k], preferred_element_type=jnp.float32).astype(jnp.bfloat16)
                for left in lefts
            ]
            for at, (out_ref, _, lanes) in enumerate(takers):
                if joint:
                    out_ref[:, lanes] = products[0][at * token_count : (at + 1) * token_count]
                else:
                    out_ref[:, lanes] = products[at]


def project(owner, features, kv_weight, wanted, head_cols, width, repeats, after=()):
    samples_here, token_count, depth = features.shape
    ranks = len({rank for rank, _ in wanted})
    panels = len({panel for _, row in wanted for panel in row})
    work = sum(len(row) for _, row in wanted)
    splits = 2
    hbm = pl.BlockSpec(memory_space=pltpu.HBM)
    return pl.pallas_call(
        functools.partial(
            project_body,
            samples_here,
            lax.axis_size("dp"),
            repeats,
            wanted,
            head_cols,
            len(after),
            splits,
        ),
        in_specs=[pl.BlockSpec(memory_space=pltpu.SMEM), hbm, hbm]
        + [pl.BlockSpec(memory_space=pl.ANY)] * len(after),
        out_specs=[pl.BlockSpec(memory_space=pltpu.VMEM)] * len(wanted),
        out_shape=[
            jax.ShapeDtypeStruct((token_count, width * len(row)), jnp.bfloat16)
            for _, row in wanted
        ],
        scratch_shapes=[
            pltpu.VMEM((ranks, token_count, depth), jnp.bfloat16),
            pltpu.VMEM((panels, depth, width), jnp.bfloat16),
            pltpu.SemaphoreType.DMA((ranks, splits)),
            pltpu.SemaphoreType.DMA((panels,)),
        ],
        cost_estimate=pl.CostEstimate(
            flops=2 * work * token_count * depth * width,
            bytes_accessed=2 * (token_count * ranks + width * panels) * depth,
            transcendentals=0,
        ),
        compiler_params=pltpu.CompilerParams(vmem_limit_bytes=58 << 20),
        name="project",
    )(owner, features, kv_weight, *after)


def mean_square(value):
    square = value * value
    high = square.astype(jnp.bfloat16)
    low = (square - high.astype(jnp.float32)).astype(jnp.bfloat16)
    parts = jnp.concatenate([high, low], axis=1)
    ones = jnp.ones((2 * HD, HD), jnp.bfloat16)
    return jnp.dot(parts, ones, preferred_element_type=jnp.float32) * (1.0 / HD)


def plan_body(samples_here, dp_count, count, owner_ref, *refs):
    shift_refs = refs[3 * count :]
    for rank, shift_ref in enumerate(shift_refs):
        slot = ranked_slot(rank, owner_ref, samples_here, dp_count)
        shift_ref[0] = lax.div(owner_ref[slot], jnp.int32(samples_here))
    add_body(*refs[: 3 * count])


def add_body(*refs):
    count = len(refs) // 3
    for k in range(count):
        ref, other, out_ref = refs[2 * k], refs[2 * k + 1], refs[2 * count + k]
        cols = out_ref.shape[1]
        out_ref[...] = (
            ref[:, cols:].astype(jnp.float32) + other[:, cols:].astype(jnp.float32)
        ).astype(jnp.bfloat16)


def add_halves(pairs, owner=None, samples_here=0):
    vmem = pl.BlockSpec(memory_space=pltpu.VMEM)
    smem = pl.BlockSpec(memory_space=pltpu.SMEM)
    shapes = [jax.ShapeDtypeStruct((p.shape[0], p.shape[1] // 2), p.dtype) for p, _ in pairs]
    body, operands = add_body, [part for pair in pairs for part in pair]
    if owner is not None:
        body = functools.partial(plan_body, samples_here, lax.axis_size("dp"), len(pairs))
        operands = [owner] + operands
    return pl.pallas_call(
        body,
        in_specs=[smem] * (owner is not None) + [vmem] * (2 * len(pairs)),
        out_specs=[vmem] * len(pairs) + [smem] * samples_here,
        out_shape=shapes + [jax.ShapeDtypeStruct((1,), jnp.int32)] * samples_here,
        cost_estimate=pl.CostEstimate(
            flops=sum(shape.size for shape in shapes),
            bytes_accessed=6 * sum(shape.size for shape in shapes),
            transcendentals=0,
        ),
        compiler_params=pltpu.CompilerParams(vmem_limit_bytes=16 << 20),
        name="add_halves",
    )(*operands)


def combine_body(layout, gain_ref, *refs):
    out_ref = refs[-1]
    gain = gain_ref[...]
    at = 0
    for head, count in enumerate(layout):
        part_refs = refs[at : at + count]
        at += count
        rows = out_ref.shape[0]
        tile = 128 if rows % 128 == 0 else rows

        def step(i, carry):
            here = pl.ds(pl.multiple_of(i * tile, tile), tile)
            for column in (0, HD):
                lanes = slice(column, column + HD)
                total = part_refs[0][here, lanes].astype(jnp.float32)
                for ref in part_refs[1:]:
                    total = total + ref[here, lanes].astype(jnp.float32)
                if column == 0:
                    total = total * lax.rsqrt(mean_square(total) + EPS) * gain
                lanes = slice(2 * HD * head + column, 2 * HD * head + column + HD)
                out_ref[here, lanes] = total.astype(jnp.bfloat16)
            return carry

        lax.fori_loop(0, rows // tile, step, 0)


def combine(k_gain, heads):
    rows = heads[0][0].shape[0]
    parts = [part for head in heads for part in head]
    vmem = pl.BlockSpec(memory_space=pltpu.VMEM)
    return pl.pallas_call(
        functools.partial(combine_body, [len(head) for head in heads]),
        in_specs=[vmem] * (len(parts) + 1),
        out_specs=vmem,
        out_shape=jax.ShapeDtypeStruct((rows, 2 * HD * len(heads)), jnp.bfloat16),
        cost_estimate=pl.CostEstimate(
            flops=2 * rows * HD * (len(parts) + 4),
            bytes_accessed=4 * rows * HD * (len(parts) + len(heads)),
            transcendentals=rows * len(heads),
        ),
        compiler_params=pltpu.CompilerParams(vmem_limit_bytes=16 << 20),
        name="combine",
    )(k_gain, *parts)


def prepare_body(gain_ref, query_ref, out_ref):
    gain = gain_ref[...] * (1.0 / math.sqrt(HD))
    rows, cols = query_ref.shape
    tile = 224 if rows % 224 == 0 else rows

    def step(i, carry):
        here = pl.ds(pl.multiple_of(i * tile, tile), tile)
        for column in range(0, cols, HD):
            head = query_ref[here, column : column + HD].astype(jnp.float32)
            out_ref[here, column : column + HD] = (
                head * lax.rsqrt(mean_square(head) + EPS) * gain
            ).astype(jnp.bfloat16)
        return carry

    lax.fori_loop(0, rows // tile, step, 0)


def prepare(q_gain, queries):
    rows, cols = queries.shape
    tile = cols // 8 if cols % (8 * HD) == 0 else cols
    block = pl.BlockSpec((rows, tile), lambda i: (0, i))
    return pl.pallas_call(
        prepare_body,
        grid=(cols // tile,),
        in_specs=[pl.BlockSpec((1, HD), lambda i: (0, 0)), block],
        out_specs=block,
        out_shape=jax.ShapeDtypeStruct((rows, cols), jnp.bfloat16),
        cost_estimate=pl.CostEstimate(
            flops=rows * cols * 6, bytes_accessed=4 * rows * cols, transcendentals=rows * cols // HD
        ),
        compiler_params=pltpu.CompilerParams(vmem_limit_bytes=24 << 20),
        name="prepare",
    )(q_gain, queries)


def attend_body(rank, samples_here, dp_count, group, last, owner_ref, counts_ref, query_ref, kv_ref, *refs):
    token_count = kv_ref.shape[0]
    cols = query_ref.shape[1]
    text_len = query_ref.shape[0] // samples_here
    slot = ranked_slot(rank, owner_ref, samples_here, dp_count)
    if last:
        earlier, (out_hbm, out_ref, sems) = refs[: samples_here - 1], refs[samples_here - 1 :]

        def rows_of(rank):
            at = ranked_slot(rank, owner_ref, samples_here, dp_count) * text_len
            return pl.ds(pl.multiple_of(at, text_len), text_len)

        copies = [
            pltpu.make_async_copy(ref, out_hbm.at[rows_of(k)], sems.at[k])
            for k, ref in enumerate(earlier)
        ]
    else:
        (out_ref,) = refs
        copies = []
    for copy in copies:
        copy.start()
    shift = lax.div(owner_ref[slot], jnp.int32(samples_here))
    source = lax.axis_index("dp").astype(jnp.int32) - shift
    source = jnp.where(source < 0, source + dp_count, source)
    images = counts_ref[source * samples_here + slot]
    keep = lax.broadcasted_iota(jnp.int32, (token_count, HD), 0) < images * PATCH
    zero = jnp.zeros((token_count, HD), jnp.float32)
    ones = jnp.where(keep, zero + 1.0, zero).astype(jnp.bfloat16)
    queries_at = pl.ds(pl.multiple_of(slot * text_len, text_len), text_len)
    stack = 2 if last and group % 2 == 0 else 4 if group % 4 == 0 else 1
    steps = group // stack
    wide = stack * HD

    def step(i, carry):
        column = i // steps * (2 * HD)
        at = i * wide
        if not last:
            column = pl.multiple_of(lax.div(i, jnp.int32(steps)) * (2 * HD), 2 * HD)
            at = pl.multiple_of(at, wide)
        key = kv_ref[:, pl.ds(column, HD)]
        value = jnp.where(
            keep, kv_ref[:, pl.ds(column + HD, HD)].astype(jnp.float32), zero
        ).astype(jnp.bfloat16)
        lanes = pl.ds(at, wide)
        queries = query_ref[queries_at, lanes]
        scores = lax.dot_general(
            jnp.concatenate([queries[:, k * HD : (k + 1) * HD] for k in range(stack)], axis=0),
            key,
            (((1,), (1,)), ((), ())),
            preferred_element_type=jnp.float32,
        )
        exponent = jnp.exp(scores).astype(jnp.bfloat16)
        summed = jnp.dot(
            exponent, jnp.concatenate([value, ones], axis=1), preferred_element_type=jnp.float32
        )
        context = (summed[:, :HD] / summed[:, HD:]).astype(jnp.bfloat16)
        out_ref[:, lanes] = jnp.concatenate(
            [context[k * text_len : (k + 1) * text_len] for k in range(stack)], axis=1
        )
        return carry

    if last:
        for i in range(cols // wide):
            step(i, 0)
            if (i + 1) % steps == 0:
                lanes = pl.ds((i + 1 - steps) * wide, steps * wide)
                copies.append(
                    pltpu.make_async_copy(
                        out_ref.at[:, lanes], out_hbm.at[rows_of(rank), lanes], sems.at[rank + i]
                    )
                )
                copies[-1].start()
    else:
        lax.fori_loop(0, cols // wide, step, 0)
    for copy in copies:
        copy.wait()


def attend(owner, counts, query_normed, kv, earlier, rank, samples_here, group):
    rows, cols = query_normed.shape
    token_count, kv_cols = kv.shape
    text_len = rows // samples_here
    last = rank == samples_here - 1
    heads = cols // HD
    smem = pl.BlockSpec(memory_space=pltpu.SMEM)
    vmem = pl.BlockSpec(memory_space=pltpu.VMEM)
    return pl.pallas_call(
        functools.partial(attend_body, rank, samples_here, lax.axis_size("dp"), group, last),
        in_specs=[smem, smem] + [vmem] * (2 + len(earlier)),
        out_specs=pl.BlockSpec(memory_space=pltpu.HBM) if last else vmem,
        out_shape=pltpu.HBM((rows, cols), jnp.bfloat16)
        if last
        else jax.ShapeDtypeStruct((text_len, cols), jnp.bfloat16),
        scratch_shapes=[
            pltpu.VMEM((text_len, cols), jnp.bfloat16),
            pltpu.SemaphoreType.DMA((samples_here - 1 + heads,)),
        ]
        * last,
        cost_estimate=pl.CostEstimate(
            flops=6 * heads * text_len * token_count * HD,
            bytes_accessed=4 * text_len * cols + 2 * token_count * kv_cols,
            transcendentals=heads * text_len * token_count,
        ),
        compiler_params=pltpu.CompilerParams(vmem_limit_bytes=ATTEND_KIB << 10),
        name="attend",
    )(owner, counts, query_normed, kv, *earlier)


def moved(value, by):
    length = lax.axis_size("dp")
    if by % length == 0:
        return value
    return lax.ppermute(value, "dp", [(i, (i + by) % length) for i in range(length)])


def by_shift(shift, start, finish):
    length = lax.axis_size("dp")
    digits = []
    unit = 1
    while unit < length:
        digits.append((unit, min(DIGIT, -(-length // unit))))
        unit *= digits[-1][1]
    if not digits:
        return finish(start(), lambda value: value)

    def choose(unit, choices, work):
        digit = shift
        if unit > 1:
            digit = lax.div(digit, jnp.int32(unit))
        if unit * choices < length:
            digit = lax.rem(digit, jnp.int32(choices))
        return conditionals._switch_internal(
            digit,
            [functools.partial(work, unit * k) for k in range(choices)],
            (),
            branches_platforms=None,
        )

    state = None
    for unit, choices in digits[:-1]:
        held = state

        def work(by):
            return moved(start() if held is None else held, by)

        state = choose(unit, choices, work)
    held = state

    def work(by):
        return finish(start() if held is None else held, lambda value: moved(value, by))

    return choose(*digits[-1], work)


def shards(queries, features, kv_weight, q_gain, k_gain, counts, owner):
    samples_here, token_count, _ = features.shape
    tensor_count = lax.axis_size("tensor")
    local_width = kv_weight.shape[1] // tensor_count
    repeats = max(1, 2 * HD // local_width)
    head_cols = local_width * repeats
    group = queries.shape[1] // HD // (head_cols // (2 * HD))
    k_gain = k_gain.reshape(1, HD)
    q_gain = q_gain.reshape(1, HD)
    dp_count = lax.axis_size("dp")

    def partials(wanted, width, after=()):
        return project(owner, features, kv_weight, wanted, head_cols, width, repeats, after)

    def swapped(part, bits):
        return lax.ppermute(part, "tensor", [(i, i ^ bits) for i in range(tensor_count)])

    def attention(rank, kv, earlier):
        return attend(owner, counts, query_normed, kv, earlier, rank, samples_here, group)

    ranks = range(samples_here)
    if tensor_count == 4 and head_cols == 4 * HD:
        def sent_of(rank):
            return [(rank, ((1, 0), (3, 0))), (rank, ((2, 1), (3, 1)))]

        def kept_of(rank):
            return [(rank, ((0, 0), (2, 0))), (rank, ((0, 1), (1, 1)))]

        sent = {0: partials(sent_of(0), 2 * HD)}

        def first(rank):
            return [swapped(part, 1 + k) for k, part in enumerate(sent[rank])]

        def second(rank, got):
            added = add_halves(list(zip(kept[rank], got)))
            return [swapped(part, 2 - k) for k, part in enumerate(added)]

        def settled(rank, got, then):
            return combine(k_gain, list(zip(kept[rank], got, then)))

        got = first(0)
        results = partials([w for rank in ranks for w in kept_of(rank)], 2 * HD)
        kept = {rank: results[2 * rank : 2 * rank + 2] for rank in ranks}
        *added, shift_a, shift_b = add_halves(list(zip(kept[0], got)), owner, samples_here)
        shifts = [shift_a.reshape(()), shift_b.reshape(())]
        then = [swapped(part, 2 - k) for k, part in enumerate(added)]
        results = partials([w for rank in ranks[1:] for w in sent_of(rank)], 2 * HD, (added[0],))
        for rank in ranks[1:]:
            sent[rank] = results[2 * rank - 2 : 2 * rank]
    else:
        blocks = list(range(tensor_count - 1, -1, -1))
        heads = range(head_cols // (2 * HD))
        sent = {
            rank: partials([(rank, ((block, head),)) for block in blocks for head in heads], 2 * HD)
            for rank in ranks
        }

        def first(rank):
            count = len(sent[rank]) - len(heads)
            return [swapped(part, blocks[k // len(heads)]) for k, part in enumerate(sent[rank][:count])]

        def second(rank, got):
            return []

        def settled(rank, got, then):
            mine = sent[rank][-len(heads) :]
            return combine(k_gain, [[mine[h]] + got[h :: len(heads)] for h in heads])

        got = first(0)
        then = []
        near = owner[:samples_here] // samples_here
        shifts = [near[rank] for rank in ranks]
        if samples_here == 2:
            reach = jnp.minimum(near, dp_count - near)
            swap = reach[1] > reach[0]
            shifts = [jnp.where(swap, near[1], near[0]), jnp.where(swap, near[0], near[1])]

    kv = ready = query_normed = None
    earlier = []
    for rank in ranks:
        held, done, known = kv, list(earlier), ready
        last = rank == samples_here - 1

        def start():
            return settled(0, got, then) if known is None else known

        def finish(value, move):
            if not last:
                coming = first(rank + 1)
            value = move(value)
            result = prepare(q_gain, queries) if rank == 0 else attention(rank - 1, held, [])
            if last:
                return attention(rank, value, done + [result])
            return value, settled(rank + 1, coming, second(rank + 1, coming)), result

        moving = by_shift(shifts[rank], start, finish)
        if last:
            return moving
        kv, ready, result = moving
        if rank == 0:
            query_normed = result
        else:
            earlier.append(result)


def solution(mesh):
    placed = (P("dp", "tensor"), P("dp", None, "tensor"), P("tensor", None), P(), P(), P(), P())
    return jax.shard_map(
        shards, mesh=mesh, in_specs=placed, out_specs=P("dp", "tensor"), check_vma=False
    )
```

```python
import functools
import math

import jax
import jax.numpy as jnp
from jax import lax
from jax._src.lax.control_flow import conditionals
from jax.experimental import pallas as pl
from jax.experimental.pallas import tpu as pltpu
from jax.sharding import PartitionSpec as P

HD = 128
PATCH = 24
EPS = 1e-05
DIGIT = 8


def ranked_slot(rank, owner_ref, samples_here, dp_count):
    if samples_here != 2:
        return rank
    reach = []
    for j in range(2):
        shift = lax.div(owner_ref[j], jnp.int32(2))
        reach.append(jnp.minimum(shift, dp_count - shift))
    return jnp.where(reach[1] > reach[0], 1 - rank, rank)


def project_body(samples_here, dp_count, repeats, wanted, head_cols, waits, splits, owner_ref, feature_hbm, weight_hbm, *rest):
    rest = rest[waits:]
    out_refs = rest[: len(wanted)]
    features, weights, feature_sem, weight_sem = rest[-4:]
    for rank, shift_ref in enumerate(rest[len(wanted) : -4]):
        slot = ranked_slot(rank, owner_ref, samples_here, dp_count)
        shift_ref[0] = lax.div(owner_ref[slot], jnp.int32(samples_here))
    me = lax.axis_index("tensor").astype(jnp.int32)
    ranks = list(dict.fromkeys(rank for rank, _ in wanted))
    rows = list(dict.fromkeys(row for _, row in wanted))
    panels = [panel for row in rows for panel in row]
    width = weights.shape[2]
    token_count, depth = features.shape[1:]
    split = token_count // splits

    def feature_copy(k, part):
        slot = ranked_slot(ranks[k], owner_ref, samples_here, dp_count)
        at = pl.ds(part * split, split)
        return pltpu.make_async_copy(
            feature_hbm.at[slot, at], features.at[k, at], feature_sem.at[k, part]
        )

    def weight_copy(k):
        block, piece = panels[k]
        head = lax.div(jnp.bitwise_xor(me, block), jnp.int32(repeats))
        start = pl.multiple_of(head * head_cols + piece * width, width)
        return pltpu.make_async_copy(
            weight_hbm.at[:, pl.ds(start, width)], weights.at[k], weight_sem.at[k]
        )

    feature_copies = [
        [feature_copy(k, part) for part in range(splits)] for k in range(len(ranks))
    ]
    weight_copies = [weight_copy(k) for k in range(len(panels))]
    ahead = 2
    for copy in feature_copies[0] + weight_copies[:ahead]:
        copy.start()
    for copies in feature_copies[1:]:
        for copy in copies:
            copy.start()
    for copies in feature_copies:
        for copy in copies:
            copy.wait()
    for copy in weight_copies[ahead:]:
        copy.start()
    base = 0
    for row in rows:
        takers = [(ref, ranks.index(rank)) for ref, (rank, taken) in zip(out_refs, wanted) if taken == row]
        joint = len(takers) > 1 and [r for _, r in takers] == list(range(len(ranks)))

        def step(p, carry, takers=takers, joint=joint, base=base):
            k = base + p
            pltpu.make_async_copy(
                weight_hbm.at[:, pl.ds(0, width)], weights.at[k], weight_sem.at[k]
            ).wait()
            lanes = pl.ds(pl.multiple_of(p * width, width), width)
            lefts = [features[...].reshape(-1, depth)] if joint else [features[r] for _, r in takers]
            products = [
                jnp.dot(left, weights[k], preferred_element_type=jnp.float32).astype(jnp.bfloat16)
                for left in lefts
            ]
            for at, (out_ref, _) in enumerate(takers):
                if joint:
                    out_ref[:, lanes] = products[0][at * token_count : (at + 1) * token_count]
                else:
                    out_ref[:, lanes] = products[at]
            return carry

        lax.fori_loop(0, len(row), step, 0)
        base += len(row)


def project(owner, features, kv_weight, wanted, head_cols, width, repeats, after=(), plan=False):
    samples_here, token_count, depth = features.shape
    ranks = len({rank for rank, _ in wanted})
    panels = len({panel for _, row in wanted for panel in row})
    work = sum(len(row) for _, row in wanted)
    splits = 2
    hbm = pl.BlockSpec(memory_space=pltpu.HBM)
    return pl.pallas_call(
        functools.partial(
            project_body,
            samples_here,
            lax.axis_size("dp"),
            repeats,
            wanted,
            head_cols,
            len(after),
            splits,
        ),
        in_specs=[pl.BlockSpec(memory_space=pltpu.SMEM), hbm, hbm]
        + [pl.BlockSpec(memory_space=pl.ANY)] * len(after),
        out_specs=[pl.BlockSpec(memory_space=pltpu.VMEM)] * len(wanted)
        + [pl.BlockSpec(memory_space=pltpu.SMEM)] * (samples_here * plan),
        out_shape=[
            jax.ShapeDtypeStruct((token_count, width * len(row)), jnp.bfloat16)
            for _, row in wanted
        ]
        + [jax.ShapeDtypeStruct((1,), jnp.int32)] * (samples_here * plan),
        scratch_shapes=[
            pltpu.VMEM((ranks, token_count, depth), jnp.bfloat16),
            pltpu.VMEM((panels, depth, width), jnp.bfloat16),
            pltpu.SemaphoreType.DMA((ranks, splits)),
            pltpu.SemaphoreType.DMA((panels,)),
        ],
        cost_estimate=pl.CostEstimate(
            flops=2 * work * token_count * depth * width,
            bytes_accessed=2 * (token_count * ranks + width * panels) * depth,
            transcendentals=0,
        ),
        compiler_params=pltpu.CompilerParams(vmem_limit_bytes=58 << 20),
        name="project",
    )(owner, features, kv_weight, *after)


def mean_square(value):
    square = value * value
    high = square.astype(jnp.bfloat16)
    low = (square - high.astype(jnp.float32)).astype(jnp.bfloat16)
    parts = jnp.concatenate([high, low], axis=1)
    ones = jnp.ones((2 * HD, HD), jnp.bfloat16)
    return jnp.dot(parts, ones, preferred_element_type=jnp.float32) * (1.0 / HD)


def add_body(*refs):
    count = len(refs) // 3
    for k in range(count):
        ref, other, out_ref = refs[2 * k], refs[2 * k + 1], refs[2 * count + k]
        cols = out_ref.shape[1]
        out_ref[...] = (
            ref[:, cols:].astype(jnp.float32) + other[:, cols:].astype(jnp.float32)
        ).astype(jnp.bfloat16)


def add_halves(pairs):
    vmem = pl.BlockSpec(memory_space=pltpu.VMEM)
    shapes = [jax.ShapeDtypeStruct((p.shape[0], p.shape[1] // 2), p.dtype) for p, _ in pairs]
    return pl.pallas_call(
        add_body,
        in_specs=[vmem] * (2 * len(pairs)),
        out_specs=[vmem] * len(pairs),
        out_shape=shapes,
        cost_estimate=pl.CostEstimate(
            flops=sum(shape.size for shape in shapes),
            bytes_accessed=6 * sum(shape.size for shape in shapes),
            transcendentals=0,
        ),
        compiler_params=pltpu.CompilerParams(vmem_limit_bytes=16 << 20),
        name="add_halves",
    )(*[part for pair in pairs for part in pair])


def combine_body(layout, gain_ref, *refs):
    out_refs = refs[sum(layout) :]
    gain = gain_ref[...]
    at = 0
    for head, count in enumerate(layout):
        part_refs = refs[at : at + count]
        at += count
        each = len(layout) // len(out_refs)
        out_ref = out_refs[head // each]
        rows = out_ref.shape[0]
        tile = 128 if rows % 128 == 0 else rows

        def step(i, carry):
            here = pl.ds(pl.multiple_of(i * tile, tile), tile)
            for column in (0, HD):
                lanes = slice(column, column + HD)
                total = part_refs[0][here, lanes].astype(jnp.float32)
                for ref in part_refs[1:]:
                    total = total + ref[here, lanes].astype(jnp.float32)
                if column == 0:
                    total = total * lax.rsqrt(mean_square(total) + EPS) * gain
                start = 2 * HD * (head % each) + column
                lanes = slice(start, start + HD)
                out_ref[here, lanes] = total.astype(jnp.bfloat16)
            return carry

        lax.fori_loop(0, rows // tile, step, 0)


def combine(k_gain, heads, outputs=1):
    rows = heads[0][0].shape[0]
    parts = [part for head in heads for part in head]
    vmem = pl.BlockSpec(memory_space=pltpu.VMEM)
    return pl.pallas_call(
        functools.partial(combine_body, [len(head) for head in heads]),
        in_specs=[vmem] * (len(parts) + 1),
        out_specs=[vmem] * outputs,
        out_shape=[jax.ShapeDtypeStruct((rows, 2 * HD * len(heads) // outputs), jnp.bfloat16)]
        * outputs,
        cost_estimate=pl.CostEstimate(
            flops=2 * rows * HD * (len(parts) + 4),
            bytes_accessed=4 * rows * HD * (len(parts) + len(heads)),
            transcendentals=rows * len(heads),
        ),
        compiler_params=pltpu.CompilerParams(vmem_limit_bytes=16 << 20),
        name="combine",
    )(k_gain, *parts)


def prepare_body(gain_ref, query_ref, out_ref):
    gain = gain_ref[...] * (1.0 / math.sqrt(HD))
    rows, cols = query_ref.shape
    tile = 224 if rows % 224 == 0 else rows

    def step(i, carry):
        here = pl.ds(pl.multiple_of(i * tile, tile), tile)
        for column in range(0, cols, HD):
            head = query_ref[here, column : column + HD].astype(jnp.float32)
            out_ref[here, column : column + HD] = (
                head * lax.rsqrt(mean_square(head) + EPS) * gain
            ).astype(jnp.bfloat16)
        return carry

    lax.fori_loop(0, rows // tile, step, 0)


def prepare(q_gain, queries):
    rows, cols = queries.shape
    tile = cols // 8 if cols % (8 * HD) == 0 else cols
    block = pl.BlockSpec((rows, tile), lambda i: (0, i))
    return pl.pallas_call(
        prepare_body,
        grid=(cols // tile,),
        in_specs=[pl.BlockSpec((1, HD), lambda i: (0, 0)), block],
        out_specs=block,
        out_shape=jax.ShapeDtypeStruct((rows, cols), jnp.bfloat16),
        cost_estimate=pl.CostEstimate(
            flops=rows * cols * 6, bytes_accessed=4 * rows * cols, transcendentals=rows * cols // HD
        ),
        compiler_params=pltpu.CompilerParams(vmem_limit_bytes=24 << 20),
        name="prepare",
    )(q_gain, queries)


def attend_body(rank, samples_here, dp_count, group, first, begins, owner_ref, counts_ref, query_ref, kv_ref, *refs):
    token_count, kv_cols = kv_ref.shape
    text_len = query_ref.shape[0] // samples_here
    cols = kv_cols // (2 * HD) * group * HD
    start = first * group * HD
    last = rank == samples_here - 1
    slot = ranked_slot(rank, owner_ref, samples_here, dp_count)

    def rows_of(rank):
        at = ranked_slot(rank, owner_ref, samples_here, dp_count) * text_len
        return pl.ds(pl.multiple_of(at, text_len), text_len)

    copies = []
    if last:
        out_hbm, out_ref, sems = refs[-3:]
        if begins:
            for k, ref in enumerate(refs[:-3]):
                copies.append(pltpu.make_async_copy(ref, out_hbm.at[rows_of(k)], sems.at[k]))
    else:
        (out_ref,) = refs
    for copy in copies:
        copy.start()
    shift = lax.div(owner_ref[slot], jnp.int32(samples_here))
    source = lax.axis_index("dp").astype(jnp.int32) - shift
    source = jnp.where(source < 0, source + dp_count, source)
    images = counts_ref[source * samples_here + slot]
    keep = lax.broadcasted_iota(jnp.int32, (token_count, HD), 0) < images * PATCH
    zero = jnp.zeros((token_count, HD), jnp.float32)
    ones = jnp.where(keep, zero + 1.0, zero).astype(jnp.bfloat16)
    queries_at = rows_of(rank)
    stack = 2 if last and group % 2 == 0 else 4 if group % 4 == 0 else 1
    steps = group // stack
    wide = stack * HD

    def step(i, carry):
        column = i // steps * (2 * HD)
        at = i * wide
        if not last:
            column = pl.multiple_of(lax.div(i, jnp.int32(steps)) * (2 * HD), 2 * HD)
            at = pl.multiple_of(at, wide)
        key = kv_ref[:, pl.ds(column, HD)]
        value = jnp.where(
            keep, kv_ref[:, pl.ds(column + HD, HD)].astype(jnp.float32), zero
        ).astype(jnp.bfloat16)
        queries = query_ref[queries_at, pl.ds(start + at, wide)]
        scores = lax.dot_general(
            jnp.concatenate([queries[:, k * HD : (k + 1) * HD] for k in range(stack)], axis=0),
            key,
            (((1,), (1,)), ((), ())),
            preferred_element_type=jnp.float32,
        )
        exponent = jnp.exp(scores).astype(jnp.bfloat16)
        summed = jnp.dot(
            exponent, jnp.concatenate([value, ones], axis=1), preferred_element_type=jnp.float32
        )
        context = (summed[:, :HD] / summed[:, HD:]).astype(jnp.bfloat16)
        out_ref[:, pl.ds(at, wide)] = jnp.concatenate(
            [context[k * text_len : (k + 1) * text_len] for k in range(stack)], axis=1
        )
        return carry

    if last:
        for i in range(cols // wide):
            step(i, 0)
        copies.append(
            pltpu.make_async_copy(
                out_ref, out_hbm.at[rows_of(rank), pl.ds(start, cols)], sems.at[rank]
            )
        )
        copies[-1].start()
    else:
        lax.fori_loop(0, cols // wide, step, 0)
    for copy in copies:
        copy.wait()


def attend(owner, counts, query_normed, kv, first, base, earlier, rank, samples_here, group):
    rows, cols = query_normed.shape
    token_count, kv_cols = kv.shape
    text_len = rows // samples_here
    last = rank == samples_here - 1
    heads = kv_cols // (2 * HD) * group
    smem = pl.BlockSpec(memory_space=pltpu.SMEM)
    vmem = pl.BlockSpec(memory_space=pltpu.VMEM)
    hbm = pl.BlockSpec(memory_space=pltpu.HBM)
    extra = list(earlier) if base is None else [base]
    return pl.pallas_call(
        functools.partial(
            attend_body, rank, samples_here, lax.axis_size("dp"), group, first, base is None
        ),
        in_specs=[smem, smem, vmem, vmem] + [vmem if base is None else hbm] * len(extra),
        out_specs=hbm if last else vmem,
        out_shape=pltpu.HBM((rows, cols), jnp.bfloat16)
        if last
        else jax.ShapeDtypeStruct((text_len, cols), jnp.bfloat16),
        input_output_aliases={} if base is None else {4: 0},
        scratch_shapes=[
            pltpu.VMEM((text_len, heads * HD), jnp.bfloat16),
            pltpu.SemaphoreType.DMA((samples_here,)),
        ]
        * last,
        cost_estimate=pl.CostEstimate(
            flops=6 * heads * text_len * token_count * HD,
            bytes_accessed=4 * text_len * heads * HD + 2 * token_count * kv_cols,
            transcendentals=heads * text_len * token_count,
        ),
        compiler_params=pltpu.CompilerParams(vmem_limit_bytes=24 << 20),
        name="attend",
    )(owner, counts, query_normed, kv, *extra)


def moved(values, by):
    length = lax.axis_size("dp")
    if by % length == 0:
        return list(values)
    pairs = [(i, (i + by) % length) for i in range(length)]
    return [lax.ppermute(value, "dp", pairs) for value in values]


def by_shift(shift, start, finish):
    length = lax.axis_size("dp")
    digits = []
    unit = 1
    while unit < length:
        digits.append((unit, min(DIGIT, -(-length // unit))))
        unit *= digits[-1][1]
    if not digits:
        return finish(start(), lambda value: value)

    def choose(unit, choices, work):
        digit = shift
        if unit > 1:
            digit = lax.div(digit, jnp.int32(unit))
        if unit * choices < length:
            digit = lax.rem(digit, jnp.int32(choices))
        return conditionals._switch_internal(
            digit,
            [functools.partial(work, unit * k) for k in range(choices)],
            (),
            branches_platforms=None,
        )

    state = None
    for unit, choices in digits[:-1]:
        held = state

        def work(by):
            return moved(start() if held is None else held, by)

        state = choose(unit, choices, work)
    held = state

    def work(by):
        return finish(start() if held is None else held, lambda value: moved(value, by))

    return choose(*digits[-1], work)


def shards(queries, features, kv_weight, q_gain, k_gain, counts, owner):
    samples_here, token_count, _ = features.shape
    tensor_count = lax.axis_size("tensor")
    local_width = kv_weight.shape[1] // tensor_count
    repeats = max(1, 2 * HD // local_width)
    head_cols = local_width * repeats
    group = queries.shape[1] // HD // (head_cols // (2 * HD))
    k_gain = k_gain.reshape(1, HD)
    q_gain = q_gain.reshape(1, HD)
    dp_count = lax.axis_size("dp")

    def partials(wanted, width, after=(), plan=False):
        return project(owner, features, kv_weight, wanted, head_cols, width, repeats, after, plan)

    def swapped(part, bits):
        return lax.ppermute(part, "tensor", [(i, i ^ bits) for i in range(tensor_count)])

    def attention(rank, kv, earlier):
        first, out = 0, None
        for part in kv:
            out = attend(
                owner, counts, query_normed, part, first, out, earlier, rank, samples_here, group
            )
            first += part.shape[1] // (2 * HD)
        return out

    ranks = range(samples_here)
    if tensor_count == 4 and head_cols == 4 * HD:
        def sent_of(rank):
            return [(rank, ((1, 0), (3, 0))), (rank, ((2, 1), (3, 1)))]

        def kept_of(rank):
            return [(rank, ((0, 0), (2, 0))), (rank, ((0, 1), (1, 1)))]

        sent = {0: partials(sent_of(0), 2 * HD)}

        def first(rank):
            return [swapped(part, 1 + k) for k, part in enumerate(sent[rank])]

        def second(rank, got):
            added = add_halves(list(zip(kept[rank], got)))
            return [swapped(part, 2 - k) for k, part in enumerate(added)]

        def settled(rank, got, then):
            return combine(k_gain, list(zip(kept[rank], got, then)), 2 if rank > 0 else 1)

        got = first(0)
        results = partials([w for rank in ranks for w in kept_of(rank)], 2 * HD)
        kept = {rank: results[2 * rank : 2 * rank + 2] for rank in ranks}
        added = add_halves(list(zip(kept[0], got)))
        then = [swapped(part, 2 - k) for k, part in enumerate(added)]
        results = partials([w for rank in ranks[1:] for w in sent_of(rank)], 2 * HD, added[:1], True)
        shifts = [shift.reshape(()) for shift in results[-samples_here:]]
        for rank in ranks[1:]:
            sent[rank] = results[2 * rank - 2 : 2 * rank]
    else:
        blocks = list(range(tensor_count - 1, -1, -1))
        heads = range(head_cols // (2 * HD))
        sent = {
            rank: partials([(rank, ((block, head),)) for block in blocks for head in heads], 2 * HD)
            for rank in ranks
        }

        def first(rank):
            count = len(sent[rank]) - len(heads)
            return [swapped(part, blocks[k // len(heads)]) for k, part in enumerate(sent[rank][:count])]

        def second(rank, got):
            return []

        def settled(rank, got, then):
            mine = sent[rank][-len(heads) :]
            return combine(k_gain, [[mine[h]] + got[h :: len(heads)] for h in heads])

        got = first(0)
        then = []
        near = owner[:samples_here] // samples_here
        shifts = [near[rank] for rank in ranks]
        if samples_here == 2:
            reach = jnp.minimum(near, dp_count - near)
            swap = reach[1] > reach[0]
            shifts = [jnp.where(swap, near[1], near[0]), jnp.where(swap, near[0], near[1])]

    kv = ready = query_normed = None
    earlier = []
    for rank in ranks:
        held, done, known = kv, list(earlier), ready
        last = rank == samples_here - 1

        def start():
            return list(settled(0, got, then)) if known is None else known

        def finish(value, move):
            if not last:
                coming = first(rank + 1)
            value = move(value)
            result = prepare(q_gain, queries) if rank == 0 else attention(rank - 1, held, [])
            if last:
                return attention(rank, value, done + [result])
            return value, list(settled(rank + 1, coming, second(rank + 1, coming))), result

        moving = by_shift(shifts[rank], start, finish)
        if last:
            return moving
        kv, ready, result = moving
        if rank == 0:
            query_normed = result
        else:
            earlier.append(result)


def solution(mesh):
    placed = (P("dp", "tensor"), P("dp", None, "tensor"), P("tensor", None), P(), P(), P(), P())
    return jax.shard_map(
        shards, mesh=mesh, in_specs=placed, out_specs=P("dp", "tensor"), check_vma=False
    )
```

```python
import functools
import math

import jax
import jax.numpy as jnp
from jax import lax
from jax._src.lax.control_flow import conditionals
from jax.experimental import pallas as pl
from jax.experimental.pallas import tpu as pltpu
from jax.sharding import PartitionSpec as P

HD = 128
PATCH = 24
EPS = 1e-05
DIGIT = 8


def ranked_slot(rank, owner_ref, samples_here, dp_count):
    if samples_here != 2:
        return rank
    reach = []
    for j in range(2):
        shift = lax.div(owner_ref[j], jnp.int32(2))
        reach.append(jnp.minimum(shift, dp_count - shift))
    return jnp.where(reach[1] > reach[0], 1 - rank, rank)


def project_body(samples_here, dp_count, repeats, wanted, head_cols, waits, splits, owner_ref, feature_hbm, weight_hbm, *rest):
    rest = rest[waits:]
    out_refs = rest[: len(wanted)]
    features, weights, feature_sem, weight_sem = rest[-4:]
    for rank, shift_ref in enumerate(rest[len(wanted) : -4]):
        slot = ranked_slot(rank, owner_ref, samples_here, dp_count)
        shift_ref[0] = lax.div(owner_ref[slot], jnp.int32(samples_here))
    me = lax.axis_index("tensor").astype(jnp.int32)
    ranks = list(dict.fromkeys(rank for rank, _ in wanted))
    rows = list(dict.fromkeys(row for _, row in wanted))
    panels = [panel for row in rows for panel in row]
    width = weights.shape[2]
    token_count, depth = features.shape[1:]
    split = token_count // splits

    def feature_copy(k, part):
        slot = ranked_slot(ranks[k], owner_ref, samples_here, dp_count)
        at = pl.ds(part * split, split)
        return pltpu.make_async_copy(
            feature_hbm.at[slot, at], features.at[k, at], feature_sem.at[k, part]
        )

    def weight_copy(k):
        block, piece = panels[k]
        head = lax.div(jnp.bitwise_xor(me, block), jnp.int32(repeats))
        start = pl.multiple_of(head * head_cols + piece * width, width)
        return pltpu.make_async_copy(
            weight_hbm.at[:, pl.ds(start, width)], weights.at[k], weight_sem.at[k]
        )

    feature_copies = [
        [feature_copy(k, part) for part in range(splits)] for k in range(len(ranks))
    ]
    weight_copies = [weight_copy(k) for k in range(len(panels))]
    ahead = 2
    for copy in feature_copies[0] + weight_copies[:ahead]:
        copy.start()
    for copies in feature_copies[1:]:
        for copy in copies:
            copy.start()
    for copies in feature_copies:
        for copy in copies:
            copy.wait()
    for copy in weight_copies[ahead:]:
        copy.start()
    base = 0
    for row in rows:
        takers = [(ref, ranks.index(rank)) for ref, (rank, taken) in zip(out_refs, wanted) if taken == row]
        joint = len(takers) > 1 and [r for _, r in takers] == list(range(len(ranks)))

        def step(p, carry, takers=takers, joint=joint, base=base):
            k = base + p
            pltpu.make_async_copy(
                weight_hbm.at[:, pl.ds(0, width)], weights.at[k], weight_sem.at[k]
            ).wait()
            lanes = pl.ds(pl.multiple_of(p * width, width), width)
            lefts = [features[...].reshape(-1, depth)] if joint else [features[r] for _, r in takers]
            products = [
                jnp.dot(left, weights[k], preferred_element_type=jnp.float32).astype(jnp.bfloat16)
                for left in lefts
            ]
            for at, (out_ref, _) in enumerate(takers):
                if joint:
                    out_ref[:, lanes] = products[0][at * token_count : (at + 1) * token_count]
                else:
                    out_ref[:, lanes] = products[at]
            return carry

        lax.fori_loop(0, len(row), step, 0)
        base += len(row)


def project(owner, features, kv_weight, wanted, head_cols, width, repeats, after=(), plan=False):
    samples_here, token_count, depth = features.shape
    ranks = len({rank for rank, _ in wanted})
    panels = len({panel for _, row in wanted for panel in row})
    work = sum(len(row) for _, row in wanted)
    splits = 2
    hbm = pl.BlockSpec(memory_space=pltpu.HBM)
    return pl.pallas_call(
        functools.partial(
            project_body,
            samples_here,
            lax.axis_size("dp"),
            repeats,
            wanted,
            head_cols,
            len(after),
            splits,
        ),
        in_specs=[pl.BlockSpec(memory_space=pltpu.SMEM), hbm, hbm]
        + [pl.BlockSpec(memory_space=pl.ANY)] * len(after),
        out_specs=[pl.BlockSpec(memory_space=pltpu.VMEM)] * len(wanted)
        + [pl.BlockSpec(memory_space=pltpu.SMEM)] * (samples_here * plan),
        out_shape=[
            pltpu.VMEM((token_count, width * len(row)), jnp.bfloat16) for _, row in wanted
        ]
        + [jax.ShapeDtypeStruct((1,), jnp.int32)] * (samples_here * plan),
        scratch_shapes=[
            pltpu.VMEM((ranks, token_count, depth), jnp.bfloat16),
            pltpu.VMEM((panels, depth, width), jnp.bfloat16),
            pltpu.SemaphoreType.DMA((ranks, splits)),
            pltpu.SemaphoreType.DMA((panels,)),
        ],
        cost_estimate=pl.CostEstimate(
            flops=2 * work * token_count * depth * width,
            bytes_accessed=2 * (token_count * ranks + width * panels) * depth,
            transcendentals=0,
        ),
        compiler_params=pltpu.CompilerParams(vmem_limit_bytes=58 << 20),
        name="project",
    )(owner, features, kv_weight, *after)


def mean_square(value):
    square = value * value
    high = square.astype(jnp.bfloat16)
    low = (square - high.astype(jnp.float32)).astype(jnp.bfloat16)
    parts = jnp.concatenate([high, low], axis=1)
    ones = jnp.ones((2 * HD, HD), jnp.bfloat16)
    return jnp.dot(parts, ones, preferred_element_type=jnp.float32) * (1.0 / HD)


def add_body(*refs):
    count = len(refs) // 3
    for k in range(count):
        ref, other, out_ref = refs[2 * k], refs[2 * k + 1], refs[2 * count + k]
        cols = out_ref.shape[1]
        out_ref[...] = (
            ref[:, cols:].astype(jnp.float32) + other[:, cols:].astype(jnp.float32)
        ).astype(jnp.bfloat16)


def add_halves(pairs):
    vmem = pl.BlockSpec(memory_space=pltpu.VMEM)
    shapes = [jax.ShapeDtypeStruct((p.shape[0], p.shape[1] // 2), p.dtype) for p, _ in pairs]
    return pl.pallas_call(
        add_body,
        in_specs=[vmem] * (2 * len(pairs)),
        out_specs=[vmem] * len(pairs),
        out_shape=shapes,
        cost_estimate=pl.CostEstimate(
            flops=sum(shape.size for shape in shapes),
            bytes_accessed=6 * sum(shape.size for shape in shapes),
            transcendentals=0,
        ),
        compiler_params=pltpu.CompilerParams(vmem_limit_bytes=16 << 20),
        name="add_halves",
    )(*[part for pair in pairs for part in pair])


def combine_body(layout, gain_ref, *refs):
    out_refs = refs[sum(layout) :]
    gain = gain_ref[...]
    at = 0
    for head, count in enumerate(layout):
        part_refs = refs[at : at + count]
        at += count
        each = len(layout) // len(out_refs)
        out_ref = out_refs[head // each]
        rows = out_ref.shape[0]
        tile = 128 if rows % 128 == 0 else rows

        def step(i, carry):
            here = pl.ds(pl.multiple_of(i * tile, tile), tile)
            for column in (0, HD):
                lanes = slice(column, column + HD)
                total = part_refs[0][here, lanes].astype(jnp.float32)
                for ref in part_refs[1:]:
                    total = total + ref[here, lanes].astype(jnp.float32)
                if column == 0:
                    total = total * lax.rsqrt(mean_square(total) + EPS) * gain
                start = 2 * HD * (head % each) + column
                lanes = slice(start, start + HD)
                out_ref[here, lanes] = total.astype(jnp.bfloat16)
            return carry

        lax.fori_loop(0, rows // tile, step, 0)


def combine(k_gain, heads, outputs=1):
    rows = heads[0][0].shape[0]
    parts = [part for head in heads for part in head]
    vmem = pl.BlockSpec(memory_space=pltpu.VMEM)
    return pl.pallas_call(
        functools.partial(combine_body, [len(head) for head in heads]),
        in_specs=[vmem] * (len(parts) + 1),
        out_specs=[vmem] * outputs,
        out_shape=[jax.ShapeDtypeStruct((rows, 2 * HD * len(heads) // outputs), jnp.bfloat16)]
        * outputs,
        cost_estimate=pl.CostEstimate(
            flops=2 * rows * HD * (len(parts) + 4),
            bytes_accessed=4 * rows * HD * (len(parts) + len(heads)),
            transcendentals=rows * len(heads),
        ),
        compiler_params=pltpu.CompilerParams(vmem_limit_bytes=16 << 20),
        name="combine",
    )(k_gain, *parts)


def prepare_body(gain_ref, query_ref, out_ref):
    gain = gain_ref[...] * (1.0 / math.sqrt(HD))
    rows, cols = query_ref.shape
    tile = 224 if rows % 224 == 0 else rows

    def step(i, carry):
        here = pl.ds(pl.multiple_of(i * tile, tile), tile)
        for column in range(0, cols, HD):
            head = query_ref[here, column : column + HD].astype(jnp.float32)
            out_ref[here, column : column + HD] = (
                head * lax.rsqrt(mean_square(head) + EPS) * gain
            ).astype(jnp.bfloat16)
        return carry

    lax.fori_loop(0, rows // tile, step, 0)


def prepare(q_gain, queries):
    rows, cols = queries.shape
    tile = cols // 8 if cols % (8 * HD) == 0 else cols
    block = pl.BlockSpec((rows, tile), lambda i: (0, i))
    return pl.pallas_call(
        prepare_body,
        grid=(cols // tile,),
        in_specs=[pl.BlockSpec((1, HD), lambda i: (0, 0)), block],
        out_specs=block,
        out_shape=jax.ShapeDtypeStruct((rows, cols), jnp.bfloat16),
        cost_estimate=pl.CostEstimate(
            flops=rows * cols * 6, bytes_accessed=4 * rows * cols, transcendentals=rows * cols // HD
        ),
        compiler_params=pltpu.CompilerParams(vmem_limit_bytes=24 << 20),
        name="prepare",
    )(q_gain, queries)


def attend_body(rank, samples_here, dp_count, group, first, last, places, owner_ref, counts_ref, query_ref, kv_ref, *refs):
    token_count, kv_cols = kv_ref.shape
    text_len = query_ref.shape[0] // samples_here
    cols = kv_cols // (2 * HD) * group * HD
    start = first * group * HD
    unrolled = rank == samples_here - 1
    slot = ranked_slot(rank, owner_ref, samples_here, dp_count)

    def rows_of(rank):
        at = ranked_slot(rank, owner_ref, samples_here, dp_count) * text_len
        return pl.ds(pl.multiple_of(at, text_len), text_len)

    copies = []
    if last:
        out_hbm, out_ref, sems = refs[-3:]
        for k, (ref, (place, lane)) in enumerate(zip(refs[:-3], places)):
            there = out_hbm.at[rows_of(place), pl.ds(lane, ref.shape[1])]
            copies.append(pltpu.make_async_copy(ref, there, sems.at[k]))
    else:
        (out_ref,) = refs
    for copy in copies:
        copy.start()
    shift = lax.div(owner_ref[slot], jnp.int32(samples_here))
    source = lax.axis_index("dp").astype(jnp.int32) - shift
    source = jnp.where(source < 0, source + dp_count, source)
    images = counts_ref[source * samples_here + slot]
    keep = lax.broadcasted_iota(jnp.int32, (token_count, HD), 0) < images * PATCH
    zero = jnp.zeros((token_count, HD), jnp.float32)
    ones = jnp.where(keep, zero + 1.0, zero).astype(jnp.bfloat16)
    queries_at = rows_of(rank)
    stack = 2 if unrolled and group % 2 == 0 else 4 if group % 4 == 0 else 1
    steps = group // stack
    wide = stack * HD

    def step(i, carry):
        column = i // steps * (2 * HD)
        at = i * wide
        if not unrolled:
            column = pl.multiple_of(lax.div(i, jnp.int32(steps)) * (2 * HD), 2 * HD)
            at = pl.multiple_of(at, wide)
        key = kv_ref[:, pl.ds(column, HD)]
        value = jnp.where(
            keep, kv_ref[:, pl.ds(column + HD, HD)].astype(jnp.float32), zero
        ).astype(jnp.bfloat16)
        queries = query_ref[queries_at, pl.ds(start + at, wide)]
        scores = lax.dot_general(
            jnp.concatenate([queries[:, k * HD : (k + 1) * HD] for k in range(stack)], axis=0),
            key,
            (((1,), (1,)), ((), ())),
            preferred_element_type=jnp.float32,
        )
        exponent = jnp.exp(scores).astype(jnp.bfloat16)
        summed = jnp.dot(
            exponent, jnp.concatenate([value, ones], axis=1), preferred_element_type=jnp.float32
        )
        context = (summed[:, :HD] / summed[:, HD:]).astype(jnp.bfloat16)
        out_ref[:, pl.ds(at, wide)] = jnp.concatenate(
            [context[k * text_len : (k + 1) * text_len] for k in range(stack)], axis=1
        )
        return carry

    if unrolled:
        for i in range(cols // wide):
            step(i, 0)
    else:
        lax.fori_loop(0, cols // wide, step, 0)
    if last:
        there = out_hbm.at[rows_of(rank), pl.ds(start, cols)]
        copies.append(pltpu.make_async_copy(out_ref, there, sems.at[len(places)]))
        copies[-1].start()
    for copy in copies:
        copy.wait()


def attend(owner, counts, query_normed, kv, first, pieces, last, rank, samples_here, group):
    rows, cols = query_normed.shape
    token_count, kv_cols = kv.shape
    text_len = rows // samples_here
    heads = kv_cols // (2 * HD) * group
    pieces = pieces if last else []
    smem = pl.BlockSpec(memory_space=pltpu.SMEM)
    vmem = pl.BlockSpec(memory_space=pltpu.VMEM)
    return pl.pallas_call(
        functools.partial(
            attend_body,
            rank,
            samples_here,
            lax.axis_size("dp"),
            group,
            first,
            last,
            [piece[1:] for piece in pieces],
        ),
        in_specs=[smem, smem, vmem, vmem] + [vmem] * len(pieces),
        out_specs=pl.BlockSpec(memory_space=pltpu.HBM) if last else vmem,
        out_shape=pltpu.HBM((rows, cols), jnp.bfloat16)
        if last
        else jax.ShapeDtypeStruct((text_len, heads * HD), jnp.bfloat16),
        scratch_shapes=[
            pltpu.VMEM((text_len, heads * HD), jnp.bfloat16),
            pltpu.SemaphoreType.DMA((len(pieces) + 1,)),
        ]
        * last,
        cost_estimate=pl.CostEstimate(
            flops=6 * heads * text_len * token_count * HD,
            bytes_accessed=4 * text_len * heads * HD + 2 * token_count * kv_cols,
            transcendentals=heads * text_len * token_count,
        ),
        compiler_params=pltpu.CompilerParams(vmem_limit_bytes=24 << 20),
        name="attend",
    )(owner, counts, query_normed, kv, *[piece[0] for piece in pieces])


def moved(values, by):
    length = lax.axis_size("dp")
    if by % length == 0:
        return list(values)
    pairs = [(i, (i + by) % length) for i in range(length)]
    return [lax.ppermute(value, "dp", pairs) for value in values]


def by_shift(shift, start, finish):
    length = lax.axis_size("dp")
    digits = []
    unit = 1
    while unit < length:
        digits.append((unit, min(DIGIT, -(-length // unit))))
        unit *= digits[-1][1]
    if not digits:
        return finish(start(), lambda value: value)

    def choose(unit, choices, work):
        digit = shift
        if unit > 1:
            digit = lax.div(digit, jnp.int32(unit))
        if unit * choices < length:
            digit = lax.rem(digit, jnp.int32(choices))
        return conditionals._switch_internal(
            digit,
            [functools.partial(work, unit * k) for k in range(choices)],
            (),
            branches_platforms=None,
        )

    state = None
    for unit, choices in digits[:-1]:
        held = state

        def work(by):
            return moved(start() if held is None else held, by)

        state = choose(unit, choices, work)
    held = state

    def work(by):
        return finish(start() if held is None else held, lambda value: moved(value, by))

    return choose(*digits[-1], work)


def shards(queries, features, kv_weight, q_gain, k_gain, counts, owner):
    samples_here, token_count, _ = features.shape
    tensor_count = lax.axis_size("tensor")
    local_width = kv_weight.shape[1] // tensor_count
    repeats = max(1, 2 * HD // local_width)
    head_cols = local_width * repeats
    group = queries.shape[1] // HD // (head_cols // (2 * HD))
    k_gain = k_gain.reshape(1, HD)
    q_gain = q_gain.reshape(1, HD)
    dp_count = lax.axis_size("dp")

    def partials(wanted, width, after=(), plan=False):
        return project(owner, features, kv_weight, wanted, head_cols, width, repeats, after, plan)

    def swapped(part, bits):
        return lax.ppermute(part, "tensor", [(i, i ^ bits) for i in range(tensor_count)])

    def attention(rank, kv, pieces):
        mine = []
        head = 0
        for k, part in enumerate(kv):
            last = rank == samples_here - 1 and k == len(kv) - 1
            out = attend(
                owner,
                counts,
                query_normed,
                part,
                head,
                pieces + mine,
                last,
                rank,
                samples_here,
                group,
            )
            mine.append((out, rank, head * group * HD))
            head += part.shape[1] // (2 * HD)
        return out if last else mine

    ranks = range(samples_here)
    if tensor_count == 4 and head_cols == 4 * HD:
        def sent_of(rank):
            return [(rank, ((1, 0), (3, 0))), (rank, ((2, 1), (3, 1)))]

        def kept_of(rank):
            return [(rank, ((0, 0), (2, 0))), (rank, ((0, 1), (1, 1)))]

        sent = {0: partials(sent_of(0), 2 * HD)}

        def first(rank):
            return [swapped(part, 1 + k) for k, part in enumerate(sent[rank])]

        def second(rank, got):
            added = add_halves(list(zip(kept[rank], got)))
            return [swapped(part, 2 - k) for k, part in enumerate(added)]

        def settled(rank, got, then):
            return combine(k_gain, list(zip(kept[rank], got, then)), 2 if rank > 0 else 1)

        got = first(0)
        early = [w for rank in ranks for w in kept_of(rank)]
        results = partials(early + [sent_of(rank)[0] for rank in ranks[1:]], 2 * HD)
        kept = {rank: results[2 * rank : 2 * rank + 2] for rank in ranks}
        sent.update({rank: [results[2 * samples_here - 1 + rank]] for rank in ranks[1:]})
        added = add_halves(list(zip(kept[0], got)))
        then = [swapped(part, 2 - k) for k, part in enumerate(added)]
        results = partials([sent_of(rank)[1] for rank in ranks[1:]], 2 * HD, added[:1], True)
        shifts = [shift.reshape(()) for shift in results[-samples_here:]]
        for rank in ranks[1:]:
            sent[rank].append(results[rank - 1])
    else:
        blocks = list(range(tensor_count - 1, -1, -1))
        heads = range(head_cols // (2 * HD))
        sent = {
            rank: partials([(rank, ((block, head),)) for block in blocks for head in heads], 2 * HD)
            for rank in ranks
        }

        def first(rank):
            count = len(sent[rank]) - len(heads)
            return [swapped(part, blocks[k // len(heads)]) for k, part in enumerate(sent[rank][:count])]

        def second(rank, got):
            return []

        def settled(rank, got, then):
            mine = sent[rank][-len(heads) :]
            return combine(k_gain, [[mine[h]] + got[h :: len(heads)] for h in heads])

        got = first(0)
        then = []
        near = owner[:samples_here] // samples_here
        shifts = [near[rank] for rank in ranks]
        if samples_here == 2:
            reach = jnp.minimum(near, dp_count - near)
            swap = reach[1] > reach[0]
            shifts = [jnp.where(swap, near[1], near[0]), jnp.where(swap, near[0], near[1])]

    kv = ready = query_normed = None
    pieces = []
    for rank in ranks:
        held, done, known = kv, list(pieces), ready
        last = rank == samples_here - 1

        def start():
            return list(settled(0, got, then)) if known is None else known

        def finish(value, move):
            if not last:
                coming = first(rank + 1)
            value = move(value)
            normed, more = None, []
            if rank == 0:
                normed = prepare(q_gain, queries)
            else:
                more = attention(rank - 1, held, [])
            if last:
                return attention(rank, value, done + more)
            following = list(settled(rank + 1, coming, second(rank + 1, coming)))
            return value, following, normed, [piece[0] for piece in more]

        moving = by_shift(shifts[rank], start, finish)
        if last:
            return moving
        before = [sum(part.shape[1] for part in kv[:k]) // (2 * HD) * group * HD for k in range(len(kv or []))]
        pieces += [(array, rank - 1, lane) for array, lane in zip(moving[3], before)]
        kv, ready = moving[:2]
        if rank == 0:
            query_normed = moving[2]


def solution(mesh):
    placed = (P("dp", "tensor"), P("dp", None, "tensor"), P("tensor", None), P(), P(), P(), P())
    return jax.shard_map(
        shards, mesh=mesh, in_specs=placed, out_specs=P("dp", "tensor"), check_vma=False
    )
```

```python
import functools
import math

import jax
import jax.numpy as jnp
from jax import lax
from jax._src.lax.control_flow import conditionals
from jax.experimental import pallas as pl
from jax.experimental.pallas import tpu as pltpu
from jax.sharding import PartitionSpec as P

HD = 128
PATCH = 24
EPS = 1e-05
DIGIT = 8


def ranked_slot(rank, owner_ref, samples_here, dp_count):
    if samples_here != 2:
        return rank
    reach = []
    for j in range(2):
        shift = lax.div(owner_ref[j], jnp.int32(2))
        reach.append(jnp.minimum(shift, dp_count - shift))
    return jnp.where(reach[1] > reach[0], 1 - rank, rank)


def project_body(samples_here, dp_count, repeats, wanted, head_cols, waits, splits, plan, owner_ref, feature_hbm, weight_hbm, *rest):
    rest = rest[waits:]
    counts_ref, rest = (rest[0], rest[1:]) if plan else (None, rest)
    out_refs = rest[: len(wanted)]
    features, weights, feature_sem, weight_sem = rest[-4:]
    if plan:
        *shift_refs, place_ref = rest[len(wanted) : -4]
        for rank, shift_ref in enumerate(shift_refs):
            slot = ranked_slot(rank, owner_ref, samples_here, dp_count)
            shift = lax.div(owner_ref[slot], jnp.int32(samples_here))
            source = lax.axis_index("dp").astype(jnp.int32) - shift
            source = jnp.where(source < 0, source + dp_count, source)
            shift_ref[0] = shift
            place_ref[2 * rank] = slot
            place_ref[2 * rank + 1] = counts_ref[source * samples_here + slot]
    me = lax.axis_index("tensor").astype(jnp.int32)
    ranks = list(dict.fromkeys(rank for rank, _ in wanted))
    rows = list(dict.fromkeys(row for _, row in wanted))
    panels = [panel for row in rows for panel in row]
    width = weights.shape[2]
    token_count, depth = features.shape[1:]
    split = token_count // splits

    def feature_copy(k, part):
        slot = ranked_slot(ranks[k], owner_ref, samples_here, dp_count)
        at = pl.ds(part * split, split)
        return pltpu.make_async_copy(
            feature_hbm.at[slot, at], features.at[k, at], feature_sem.at[k, part]
        )

    def weight_copy(k):
        block, piece = panels[k]
        head = lax.div(jnp.bitwise_xor(me, block), jnp.int32(repeats))
        start = pl.multiple_of(head * head_cols + piece * width, width)
        return pltpu.make_async_copy(
            weight_hbm.at[:, pl.ds(start, width)], weights.at[k], weight_sem.at[k]
        )

    feature_copies = [
        [feature_copy(k, part) for part in range(splits)] for k in range(len(ranks))
    ]
    weight_copies = [weight_copy(k) for k in range(len(panels))]
    ahead = 2
    for copy in feature_copies[0] + weight_copies[:ahead]:
        copy.start()
    for copies in feature_copies[1:]:
        for copy in copies:
            copy.start()
    for copies in feature_copies:
        for copy in copies:
            copy.wait()
    for copy in weight_copies[ahead:]:
        copy.start()
    base = 0
    for row in rows:
        takers = [(ref, ranks.index(rank)) for ref, (rank, taken) in zip(out_refs, wanted) if taken == row]
        joint = len(takers) > 1 and [r for _, r in takers] == list(range(len(ranks)))

        def step(p, carry, takers=takers, joint=joint, base=base):
            k = base + p
            pltpu.make_async_copy(
                weight_hbm.at[:, pl.ds(0, width)], weights.at[k], weight_sem.at[k]
            ).wait()
            lanes = pl.ds(pl.multiple_of(p * width, width), width)
            lefts = [features[...].reshape(-1, depth)] if joint else [features[r] for _, r in takers]
            products = [
                jnp.dot(left, weights[k], preferred_element_type=jnp.float32).astype(jnp.bfloat16)
                for left in lefts
            ]
            for at, (out_ref, _) in enumerate(takers):
                if joint:
                    out_ref[:, lanes] = products[0][at * token_count : (at + 1) * token_count]
                else:
                    out_ref[:, lanes] = products[at]
            return carry

        lax.fori_loop(0, len(row), step, 0)
        base += len(row)


def project(owner, features, kv_weight, wanted, head_cols, width, repeats, after=(), counts=None):
    plan = counts is not None
    samples_here, token_count, depth = features.shape
    ranks = len({rank for rank, _ in wanted})
    panels = len({panel for _, row in wanted for panel in row})
    work = sum(len(row) for _, row in wanted)
    splits = 2
    hbm = pl.BlockSpec(memory_space=pltpu.HBM)
    return pl.pallas_call(
        functools.partial(
            project_body,
            samples_here,
            lax.axis_size("dp"),
            repeats,
            wanted,
            head_cols,
            len(after),
            splits,
            plan,
        ),
        in_specs=[pl.BlockSpec(memory_space=pltpu.SMEM), hbm, hbm]
        + [pl.BlockSpec(memory_space=pl.ANY)] * len(after)
        + [pl.BlockSpec(memory_space=pltpu.SMEM)] * plan,
        out_specs=[pl.BlockSpec(memory_space=pltpu.VMEM)] * len(wanted)
        + [pl.BlockSpec(memory_space=pltpu.SMEM)] * ((samples_here + 1) * plan),
        out_shape=[
            pltpu.VMEM((token_count, width * len(row)), jnp.bfloat16) for _, row in wanted
        ]
        + [pltpu.SMEM((1,), jnp.int32)] * (samples_here * plan)
        + [pltpu.SMEM((2 * samples_here,), jnp.int32)] * plan,
        scratch_shapes=[
            pltpu.VMEM((ranks, token_count, depth), jnp.bfloat16),
            pltpu.VMEM((panels, depth, width), jnp.bfloat16),
            pltpu.SemaphoreType.DMA((ranks, splits)),
            pltpu.SemaphoreType.DMA((panels,)),
        ],
        cost_estimate=pl.CostEstimate(
            flops=2 * work * token_count * depth * width,
            bytes_accessed=2 * (token_count * ranks + width * panels) * depth,
            transcendentals=0,
        ),
        compiler_params=pltpu.CompilerParams(vmem_limit_bytes=58 << 20),
        name="project",
    )(owner, features, kv_weight, *after, *([counts] * plan))


def mean_square(value):
    square = value * value
    high = square.astype(jnp.bfloat16)
    low = (square - high.astype(jnp.float32)).astype(jnp.bfloat16)
    parts = jnp.concatenate([high, low], axis=1)
    ones = jnp.ones((2 * HD, HD), jnp.bfloat16)
    return jnp.dot(parts, ones, preferred_element_type=jnp.float32) * (1.0 / HD)


def add_body(*refs):
    count = len(refs) // 3
    for k in range(count):
        ref, other, out_ref = refs[2 * k], refs[2 * k + 1], refs[2 * count + k]
        cols = out_ref.shape[1]
        out_ref[...] = (
            ref[:, cols:].astype(jnp.float32) + other[:, cols:].astype(jnp.float32)
        ).astype(jnp.bfloat16)


def add_halves(pairs):
    vmem = pl.BlockSpec(memory_space=pltpu.VMEM)
    shapes = [jax.ShapeDtypeStruct((p.shape[0], p.shape[1] // 2), p.dtype) for p, _ in pairs]
    return pl.pallas_call(
        add_body,
        in_specs=[vmem] * (2 * len(pairs)),
        out_specs=[vmem] * len(pairs),
        out_shape=shapes,
        cost_estimate=pl.CostEstimate(
            flops=sum(shape.size for shape in shapes),
            bytes_accessed=6 * sum(shape.size for shape in shapes),
            transcendentals=0,
        ),
        compiler_params=pltpu.CompilerParams(vmem_limit_bytes=16 << 20),
        name="add_halves",
    )(*[part for pair in pairs for part in pair])


def combine_body(layout, gain_ref, *refs):
    out_refs = refs[sum(layout) :]
    gain = gain_ref[...]
    at = 0
    for head, count in enumerate(layout):
        part_refs = refs[at : at + count]
        at += count
        each = len(layout) // len(out_refs)
        out_ref = out_refs[head // each]
        rows = out_ref.shape[0]
        tile = 128 if rows % 128 == 0 else rows

        def step(i, carry):
            here = pl.ds(pl.multiple_of(i * tile, tile), tile)
            for column in (0, HD):
                lanes = slice(column, column + HD)
                total = part_refs[0][here, lanes].astype(jnp.float32)
                for ref in part_refs[1:]:
                    total = total + ref[here, lanes].astype(jnp.float32)
                if column == 0:
                    total = total * lax.rsqrt(mean_square(total) + EPS) * gain
                start = 2 * HD * (head % each) + column
                lanes = slice(start, start + HD)
                out_ref[here, lanes] = total.astype(jnp.bfloat16)
            return carry

        lax.fori_loop(0, rows // tile, step, 0)


def combine(k_gain, heads, outputs=1):
    rows = heads[0][0].shape[0]
    parts = [part for head in heads for part in head]
    vmem = pl.BlockSpec(memory_space=pltpu.VMEM)
    return pl.pallas_call(
        functools.partial(combine_body, [len(head) for head in heads]),
        in_specs=[vmem] * (len(parts) + 1),
        out_specs=[vmem] * outputs,
        out_shape=[jax.ShapeDtypeStruct((rows, 2 * HD * len(heads) // outputs), jnp.bfloat16)]
        * outputs,
        cost_estimate=pl.CostEstimate(
            flops=2 * rows * HD * (len(parts) + 4),
            bytes_accessed=4 * rows * HD * (len(parts) + len(heads)),
            transcendentals=rows * len(heads),
        ),
        compiler_params=pltpu.CompilerParams(vmem_limit_bytes=16 << 20),
        name="combine",
    )(k_gain, *parts)


def prepare_body(gain_ref, query_ref, out_ref):
    gain = gain_ref[...] * (1.0 / math.sqrt(HD))
    rows, cols = query_ref.shape
    tile = 224 if rows % 224 == 0 else rows

    def step(i, carry):
        here = pl.ds(pl.multiple_of(i * tile, tile), tile)
        for column in range(0, cols, HD):
            head = query_ref[here, column : column + HD].astype(jnp.float32)
            out_ref[here, column : column + HD] = (
                head * lax.rsqrt(mean_square(head) + EPS) * gain
            ).astype(jnp.bfloat16)
        return carry

    lax.fori_loop(0, rows // tile, step, 0)


def prepare(q_gain, queries):
    rows, cols = queries.shape
    tile = cols // 8 if cols % (8 * HD) == 0 else cols
    block = pl.BlockSpec((rows, tile), lambda i: (0, i))
    return pl.pallas_call(
        prepare_body,
        grid=(cols // tile,),
        in_specs=[pl.BlockSpec((1, HD), lambda i: (0, 0)), block],
        out_specs=block,
        out_shape=jax.ShapeDtypeStruct((rows, cols), jnp.bfloat16),
        cost_estimate=pl.CostEstimate(
            flops=rows * cols * 6, bytes_accessed=4 * rows * cols, transcendentals=rows * cols // HD
        ),
        compiler_params=pltpu.CompilerParams(vmem_limit_bytes=24 << 20),
        name="prepare",
    )(q_gain, queries)


def attend_body(rank, samples_here, group, first, last, unrolled, places, place_ref, query_ref, kv_ref, *refs):
    token_count, kv_cols = kv_ref.shape
    text_len = query_ref.shape[0] // samples_here
    cols = kv_cols // (2 * HD) * group * HD
    start = first * group * HD

    def rows_of(rank):
        return pl.ds(pl.multiple_of(place_ref[2 * rank] * text_len, text_len), text_len)

    copies = []
    if last:
        out_hbm, out_ref, sems = refs[-3:]
        for k, (ref, (place, lane)) in enumerate(zip(refs[:-3], places)):
            there = out_hbm.at[rows_of(place), pl.ds(lane, ref.shape[1])]
            copies.append(pltpu.make_async_copy(ref, there, sems.at[k]))
    else:
        (out_ref,) = refs
    for copy in copies:
        copy.start()
    images = place_ref[2 * rank + 1]
    keep = lax.broadcasted_iota(jnp.int32, (token_count, HD), 0) < images * PATCH
    zero = jnp.zeros((token_count, HD), jnp.float32)
    ones = jnp.where(keep, zero + 1.0, zero).astype(jnp.bfloat16)
    queries_at = rows_of(rank)
    stack = 2 if unrolled and group % 2 == 0 else 4 if group % 4 == 0 else 1
    steps = group // stack
    wide = stack * HD

    def step(i, carry):
        column = i // steps * (2 * HD)
        at = i * wide
        if not unrolled:
            column = pl.multiple_of(lax.div(i, jnp.int32(steps)) * (2 * HD), 2 * HD)
            at = pl.multiple_of(at, wide)
        key = kv_ref[:, pl.ds(column, HD)]
        value = jnp.where(
            keep, kv_ref[:, pl.ds(column + HD, HD)].astype(jnp.float32), zero
        ).astype(jnp.bfloat16)
        queries = query_ref[queries_at, pl.ds(start + at, wide)]
        scores = lax.dot_general(
            jnp.concatenate([queries[:, k * HD : (k + 1) * HD] for k in range(stack)], axis=0),
            key,
            (((1,), (1,)), ((), ())),
            preferred_element_type=jnp.float32,
        )
        exponent = jnp.exp(scores).astype(jnp.bfloat16)
        summed = jnp.dot(
            exponent, jnp.concatenate([value, ones], axis=1), preferred_element_type=jnp.float32
        )
        context = (summed[:, :HD] / summed[:, HD:]).astype(jnp.bfloat16)
        out_ref[:, pl.ds(at, wide)] = jnp.concatenate(
            [context[k * text_len : (k + 1) * text_len] for k in range(stack)], axis=1
        )
        return carry

    if unrolled:
        for i in range(cols // wide):
            step(i, 0)
    else:
        lax.fori_loop(0, cols // wide, step, 0)
    if last:
        there = out_hbm.at[rows_of(rank), pl.ds(start, cols)]
        copies.append(pltpu.make_async_copy(out_ref, there, sems.at[len(places)]))
        copies[-1].start()
    for copy in copies:
        copy.wait()


def attend(place, query_normed, kv, first, pieces, last, unrolled, rank, samples_here, group):
    rows, cols = query_normed.shape
    token_count, kv_cols = kv.shape
    text_len = rows // samples_here
    heads = kv_cols // (2 * HD) * group
    pieces = pieces if last else []
    smem = pl.BlockSpec(memory_space=pltpu.SMEM)
    vmem = pl.BlockSpec(memory_space=pltpu.VMEM)
    return pl.pallas_call(
        functools.partial(
            attend_body,
            rank,
            samples_here,
            group,
            first,
            last,
            unrolled,
            [piece[1:] for piece in pieces],
        ),
        in_specs=[smem, vmem, vmem] + [vmem] * len(pieces),
        out_specs=pl.BlockSpec(memory_space=pltpu.HBM) if last else vmem,
        out_shape=pltpu.HBM((rows, cols), jnp.bfloat16)
        if last
        else jax.ShapeDtypeStruct((text_len, heads * HD), jnp.bfloat16),
        scratch_shapes=[
            pltpu.VMEM((text_len, heads * HD), jnp.bfloat16),
            pltpu.SemaphoreType.DMA((len(pieces) + 1,)),
        ]
        * last,
        cost_estimate=pl.CostEstimate(
            flops=6 * heads * text_len * token_count * HD,
            bytes_accessed=4 * text_len * heads * HD + 2 * token_count * kv_cols,
            transcendentals=heads * text_len * token_count,
        ),
        compiler_params=pltpu.CompilerParams(vmem_limit_bytes=24 << 20),
        name="attend",
    )(place, query_normed, kv, *[piece[0] for piece in pieces])


def moved(values, by):
    length = lax.axis_size("dp")
    if by % length == 0:
        return list(values)
    pairs = [(i, (i + by) % length) for i in range(length)]
    return [lax.ppermute(value, "dp", pairs) for value in values]


def by_shift(shift, start, finish):
    length = lax.axis_size("dp")
    digits = []
    unit = 1
    while unit < length:
        digits.append((unit, min(DIGIT, -(-length // unit))))
        unit *= digits[-1][1]
    if not digits:
        return finish(start(), lambda value: value, True)

    def choose(unit, choices, work):
        digit = shift
        if unit > 1:
            digit = lax.div(digit, jnp.int32(unit))
        if unit * choices < length:
            digit = lax.rem(digit, jnp.int32(choices))
        return conditionals._switch_internal(
            digit,
            [functools.partial(work, unit * k) for k in range(choices)],
            (),
            branches_platforms=None,
        )

    state = None
    for unit, choices in digits[:-1]:
        held = state

        def work(by):
            return moved(start() if held is None else held, by)

        state = choose(unit, choices, work)
    held = state

    def work(by):
        value = start() if held is None else held
        return finish(value, lambda value: moved(value, by), by == 0)

    return choose(*digits[-1], work)


def shards(queries, features, kv_weight, q_gain, k_gain, counts, owner):
    samples_here, token_count, _ = features.shape
    tensor_count = lax.axis_size("tensor")
    local_width = kv_weight.shape[1] // tensor_count
    repeats = max(1, 2 * HD // local_width)
    head_cols = local_width * repeats
    group = queries.shape[1] // HD // (head_cols // (2 * HD))
    k_gain = k_gain.reshape(1, HD)
    q_gain = q_gain.reshape(1, HD)

    def partials(wanted, width, after=(), counts=None):
        return project(owner, features, kv_weight, wanted, head_cols, width, repeats, after, counts)

    def swapped(part, bits):
        return lax.ppermute(part, "tensor", [(i, i ^ bits) for i in range(tensor_count)])

    def attention(rank, kv, pieces, unrolled):
        mine = []
        head = 0
        for k, part in enumerate(kv):
            last = rank == samples_here - 1 and k == len(kv) - 1
            out = attend(
                place,
                query_normed,
                part,
                head,
                pieces + mine,
                last,
                unrolled,
                rank,
                samples_here,
                group,
            )
            mine.append((out, rank, head * group * HD))
            head += part.shape[1] // (2 * HD)
        return out if last else mine

    ranks = range(samples_here)
    if tensor_count == 4 and head_cols == 4 * HD:
        def sent_of(rank):
            return [(rank, ((1, 0), (3, 0))), (rank, ((2, 1), (3, 1)))]

        def kept_of(rank):
            return [(rank, ((0, 0), (2, 0))), (rank, ((0, 1), (1, 1)))]

        sent = {0: partials(sent_of(0), 2 * HD)}

        def first(rank):
            return [swapped(part, 1 + k) for k, part in enumerate(sent[rank])]

        def second(rank, got):
            added = add_halves(list(zip(kept[rank], got)))
            return [swapped(part, 2 - k) for k, part in enumerate(added)]

        def settled(rank, got, then):
            return combine(k_gain, list(zip(kept[rank], got, then)), 2 if rank > 0 else 1)

        got = first(0)
        early = [w for rank in ranks for w in kept_of(rank)]
        results = partials(early + [sent_of(rank)[0] for rank in ranks[1:]], 2 * HD)
        kept = {rank: results[2 * rank : 2 * rank + 2] for rank in ranks}
        sent.update({rank: [results[2 * samples_here - 1 + rank]] for rank in ranks[1:]})
        added = add_halves(list(zip(kept[0], got)))
        then = [swapped(part, 2 - k) for k, part in enumerate(added)]
        results = partials([sent_of(rank)[1] for rank in ranks[1:]], 2 * HD, added[:1], counts)
        *results, place = results
        for rank in ranks[1:]:
            sent[rank].append(results[rank - 1])
    else:
        blocks = list(range(tensor_count - 1, -1, -1))
        heads = range(head_cols // (2 * HD))
        sent = {}
        for rank in ranks:
            planned = counts if rank == samples_here - 1 else None
            wanted = [(rank, ((block, head),)) for block in blocks for head in heads]
            results = partials(wanted, 2 * HD, (), planned)
            sent[rank] = results[: len(wanted)]
        *results, place = results

        def first(rank):
            count = len(sent[rank]) - len(heads)
            return [swapped(part, blocks[k // len(heads)]) for k, part in enumerate(sent[rank][:count])]

        def second(rank, got):
            return []

        def settled(rank, got, then):
            mine = sent[rank][-len(heads) :]
            return combine(k_gain, [[mine[h]] + got[h :: len(heads)] for h in heads])

        got = first(0)
        then = []

    shifts = [shift.reshape(()) for shift in results[-samples_here:]]
    kv = ready = query_normed = None
    pieces = []
    for rank in ranks:
        held, done, known = kv, list(pieces), ready
        last = rank == samples_here - 1

        def start():
            return list(settled(0, got, then)) if known is None else known

        def finish(value, move, still):
            if not last:
                coming = first(rank + 1)
            value = move(value)
            normed, more = None, []
            if rank == 0:
                normed = prepare(q_gain, queries)
            else:
                more = attention(rank - 1, held, [], still)
            if last:
                return attention(rank, value, done + more, True)
            following = list(settled(rank + 1, coming, second(rank + 1, coming)))
            return value, following, normed, [piece[0] for piece in more]

        moving = by_shift(shifts[rank], start, finish)
        if last:
            return moving
        before = [sum(part.shape[1] for part in kv[:k]) // (2 * HD) * group * HD for k in range(len(kv or []))]
        pieces += [(array, rank - 1, lane) for array, lane in zip(moving[3], before)]
        kv, ready = moving[:2]
        if rank == 0:
            query_normed = moving[2]


def solution(mesh):
    placed = (P("dp", "tensor"), P("dp", None, "tensor"), P("tensor", None), P(), P(), P(), P())
    return jax.shard_map(
        shards, mesh=mesh, in_specs=placed, out_specs=P("dp", "tensor"), check_vma=False
    )
```

```python
import functools
import math

import jax
import jax.numpy as jnp
from jax import lax
from jax._src.lax.control_flow import conditionals
from jax.experimental import pallas as pl
from jax.experimental.pallas import tpu as pltpu
from jax.sharding import PartitionSpec as P

HD = 128
PATCH = 24
EPS = 1e-05
DIGIT = 8


def ranked_slot(rank, owner_ref, samples_here, dp_count):
    if samples_here != 2:
        return rank
    reach = []
    for j in range(2):
        shift = lax.div(owner_ref[j], jnp.int32(2))
        reach.append(jnp.minimum(shift, dp_count - shift))
    return jnp.where(reach[1] > reach[0], 1 - rank, rank)


def project_body(samples_here, dp_count, repeats, wanted, head_cols, waits, splits, plan, leads, owner_ref, feature_hbm, weight_hbm, *rest):
    rest = rest[waits:]
    if plan:
        slots_ref, owner_ref, counts_ref, *rest = owner_ref, *rest
        slot_of = lambda rank: slots_ref[rank]
    elif leads:
        owner_hbm = owner_ref
        *rest, owner_ref, owner_sem = rest
        slot_of = lambda rank: ranked_slot(rank, owner_ref, samples_here, dp_count)
    else:
        slots_ref = owner_ref
        slot_of = lambda rank: slots_ref[rank]
    out_refs = rest[: len(wanted)]
    features, weights, feature_sem, weight_sem = rest[-4:]
    if plan:
        *shift_refs, place_ref = rest[len(wanted) : -4]
        for rank, shift_ref in enumerate(shift_refs):
            slot = slot_of(rank)
            shift = lax.div(owner_ref[slot], jnp.int32(samples_here))
            source = lax.axis_index("dp").astype(jnp.int32) - shift
            source = jnp.where(source < 0, source + dp_count, source)
            shift_ref[0] = shift
            place_ref[2 * rank] = slot
            place_ref[2 * rank + 1] = counts_ref[source * samples_here + slot]
    me = lax.axis_index("tensor").astype(jnp.int32)
    ranks = list(dict.fromkeys(rank for rank, _ in wanted))
    rows = list(dict.fromkeys(row for _, row in wanted))
    panels = [panel for row in rows for panel in row]
    width = weights.shape[2]
    token_count, depth = features.shape[1:]
    split = token_count // splits

    def feature_copy(k, part):
        at = pl.ds(part * split, split)
        return pltpu.make_async_copy(
            feature_hbm.at[slot_of(ranks[k]), at], features.at[k, at], feature_sem.at[k, part]
        )

    def weight_copy(k):
        block, piece = panels[k]
        head = lax.div(jnp.bitwise_xor(me, block), jnp.int32(repeats))
        start = pl.multiple_of(head * head_cols + piece * width, width)
        return pltpu.make_async_copy(
            weight_hbm.at[:, pl.ds(start, width)], weights.at[k], weight_sem.at[k]
        )

    weight_copies = [weight_copy(k) for k in range(len(panels))]
    ahead = 2
    if leads:
        owner_copy = pltpu.make_async_copy(owner_hbm, owner_ref, owner_sem)
        owner_copy.start()
    for copy in weight_copies[:ahead]:
        copy.start()
    if leads:
        owner_copy.wait()
        for rank in range(samples_here):
            rest[len(wanted)][rank] = slot_of(rank)
    feature_copies = [
        [feature_copy(k, part) for part in range(splits)] for k in range(len(ranks))
    ]
    for copy in feature_copies[0]:
        copy.start()
    for copies in feature_copies[1:]:
        for copy in copies:
            copy.start()
    for copies in feature_copies:
        for copy in copies:
            copy.wait()
    for copy in weight_copies[ahead:]:
        copy.start()
    base = 0
    for row in rows:
        takers = [(ref, ranks.index(rank)) for ref, (rank, taken) in zip(out_refs, wanted) if taken == row]
        joint = len(takers) > 1 and [r for _, r in takers] == list(range(len(ranks)))

        def step(p, carry, takers=takers, joint=joint, base=base):
            k = base + p
            pltpu.make_async_copy(
                weight_hbm.at[:, pl.ds(0, width)], weights.at[k], weight_sem.at[k]
            ).wait()
            lanes = pl.ds(pl.multiple_of(p * width, width), width)
            lefts = [features[...].reshape(-1, depth)] if joint else [features[r] for _, r in takers]
            products = [
                jnp.dot(left, weights[k], preferred_element_type=jnp.float32).astype(jnp.bfloat16)
                for left in lefts
            ]
            for at, (out_ref, _) in enumerate(takers):
                if joint:
                    out_ref[:, lanes] = products[0][at * token_count : (at + 1) * token_count]
                else:
                    out_ref[:, lanes] = products[at]
            return carry

        lax.fori_loop(0, len(row), step, 0)
        base += len(row)


def project(owner, features, kv_weight, wanted, head_cols, width, repeats, after=(), counts=None, slots=None):
    plan = counts is not None
    leads = slots is None
    samples_here, token_count, depth = features.shape
    ranks = len({rank for rank, _ in wanted})
    panels = len({panel for _, row in wanted for panel in row})
    work = sum(len(row) for _, row in wanted)
    splits = 2
    hbm = pl.BlockSpec(memory_space=pltpu.HBM)
    return pl.pallas_call(
        functools.partial(
            project_body,
            samples_here,
            lax.axis_size("dp"),
            repeats,
            wanted,
            head_cols,
            len(after),
            splits,
            plan,
            leads,
        ),
        in_specs=[hbm if leads else pl.BlockSpec(memory_space=pltpu.SMEM), hbm, hbm]
        + [pl.BlockSpec(memory_space=pl.ANY)] * len(after)
        + [pl.BlockSpec(memory_space=pltpu.SMEM)] * (2 * plan),
        out_specs=[pl.BlockSpec(memory_space=pltpu.VMEM)] * len(wanted)
        + [pl.BlockSpec(memory_space=pltpu.SMEM)] * ((samples_here + 1) * plan + leads),
        out_shape=[
            pltpu.VMEM((token_count, width * len(row)), jnp.bfloat16) for _, row in wanted
        ]
        + [pltpu.SMEM((1,), jnp.int32)] * (samples_here * plan)
        + [pltpu.SMEM((2 * samples_here,), jnp.int32)] * plan
        + [pltpu.SMEM((samples_here,), jnp.int32)] * leads,
        scratch_shapes=[
            pltpu.VMEM((ranks, token_count, depth), jnp.bfloat16),
            pltpu.VMEM((panels, depth, width), jnp.bfloat16),
            pltpu.SemaphoreType.DMA((ranks, splits)),
            pltpu.SemaphoreType.DMA((panels,)),
        ]
        + [pltpu.SMEM(owner.shape, jnp.int32), pltpu.SemaphoreType.DMA] * leads,
        cost_estimate=pl.CostEstimate(
            flops=2 * work * token_count * depth * width,
            bytes_accessed=2 * (token_count * ranks + width * panels) * depth,
            transcendentals=0,
        ),
        compiler_params=pltpu.CompilerParams(vmem_limit_bytes=58 << 20),
        name="project",
    )(owner if leads else slots, features, kv_weight, *after, *([owner, counts] * plan))


def mean_square(value):
    square = value * value
    high = square.astype(jnp.bfloat16)
    low = (square - high.astype(jnp.float32)).astype(jnp.bfloat16)
    parts = jnp.concatenate([high, low], axis=1)
    ones = jnp.ones((2 * HD, HD), jnp.bfloat16)
    return jnp.dot(parts, ones, preferred_element_type=jnp.float32) * (1.0 / HD)


def add_body(*refs):
    count = len(refs) // 3
    for k in range(count):
        ref, other, out_ref = refs[2 * k], refs[2 * k + 1], refs[2 * count + k]
        cols = out_ref.shape[1]
        out_ref[...] = (
            ref[:, cols:].astype(jnp.float32) + other[:, cols:].astype(jnp.float32)
        ).astype(jnp.bfloat16)


def add_halves(pairs):
    vmem = pl.BlockSpec(memory_space=pltpu.VMEM)
    shapes = [jax.ShapeDtypeStruct((p.shape[0], p.shape[1] // 2), p.dtype) for p, _ in pairs]
    return pl.pallas_call(
        add_body,
        in_specs=[vmem] * (2 * len(pairs)),
        out_specs=[vmem] * len(pairs),
        out_shape=shapes,
        cost_estimate=pl.CostEstimate(
            flops=sum(shape.size for shape in shapes),
            bytes_accessed=6 * sum(shape.size for shape in shapes),
            transcendentals=0,
        ),
        compiler_params=pltpu.CompilerParams(vmem_limit_bytes=16 << 20),
        name="add_halves",
    )(*[part for pair in pairs for part in pair])


def combine_body(layout, gain_ref, *refs):
    out_refs = refs[sum(layout) :]
    gain = gain_ref[...]
    at = 0
    for head, count in enumerate(layout):
        part_refs = refs[at : at + count]
        at += count
        each = len(layout) // len(out_refs)
        out_ref = out_refs[head // each]
        rows = out_ref.shape[0]
        tile = 128 if rows % 128 == 0 else rows

        def step(i, carry):
            here = pl.ds(pl.multiple_of(i * tile, tile), tile)
            for column in (0, HD):
                lanes = slice(column, column + HD)
                total = part_refs[0][here, lanes].astype(jnp.float32)
                for ref in part_refs[1:]:
                    total = total + ref[here, lanes].astype(jnp.float32)
                if column == 0:
                    total = total * lax.rsqrt(mean_square(total) + EPS) * gain
                start = 2 * HD * (head % each) + column
                lanes = slice(start, start + HD)
                out_ref[here, lanes] = total.astype(jnp.bfloat16)
            return carry

        lax.fori_loop(0, rows // tile, step, 0)


def combine(k_gain, heads, outputs=1):
    rows = heads[0][0].shape[0]
    parts = [part for head in heads for part in head]
    vmem = pl.BlockSpec(memory_space=pltpu.VMEM)
    return pl.pallas_call(
        functools.partial(combine_body, [len(head) for head in heads]),
        in_specs=[vmem] * (len(parts) + 1),
        out_specs=[vmem] * outputs,
        out_shape=[jax.ShapeDtypeStruct((rows, 2 * HD * len(heads) // outputs), jnp.bfloat16)]
        * outputs,
        cost_estimate=pl.CostEstimate(
            flops=2 * rows * HD * (len(parts) + 4),
            bytes_accessed=4 * rows * HD * (len(parts) + len(heads)),
            transcendentals=rows * len(heads),
        ),
        compiler_params=pltpu.CompilerParams(vmem_limit_bytes=16 << 20),
        name="combine",
    )(k_gain, *parts)


def prepare_body(gain_ref, query_ref, out_ref):
    gain = gain_ref[...] * (1.0 / math.sqrt(HD))
    rows, cols = query_ref.shape
    tile = 224 if rows % 224 == 0 else rows

    def step(i, carry):
        here = pl.ds(pl.multiple_of(i * tile, tile), tile)
        for column in range(0, cols, HD):
            head = query_ref[here, column : column + HD].astype(jnp.float32)
            out_ref[here, column : column + HD] = (
                head * lax.rsqrt(mean_square(head) + EPS) * gain
            ).astype(jnp.bfloat16)
        return carry

    lax.fori_loop(0, rows // tile, step, 0)


def prepare(q_gain, queries):
    rows, cols = queries.shape
    tile = cols // 8 if cols % (8 * HD) == 0 else cols
    block = pl.BlockSpec((rows, tile), lambda i: (0, i))
    return pl.pallas_call(
        prepare_body,
        grid=(cols // tile,),
        in_specs=[pl.BlockSpec((1, HD), lambda i: (0, 0)), block],
        out_specs=block,
        out_shape=jax.ShapeDtypeStruct((rows, cols), jnp.bfloat16),
        cost_estimate=pl.CostEstimate(
            flops=rows * cols * 6, bytes_accessed=4 * rows * cols, transcendentals=rows * cols // HD
        ),
        compiler_params=pltpu.CompilerParams(vmem_limit_bytes=24 << 20),
        name="prepare",
    )(q_gain, queries)


def attend_body(rank, samples_here, group, first, last, unrolled, places, place_ref, query_ref, kv_ref, *refs):
    token_count, kv_cols = kv_ref.shape
    text_len = query_ref.shape[0] // samples_here
    cols = kv_cols // (2 * HD) * group * HD
    start = first * group * HD

    def rows_of(rank):
        return pl.ds(pl.multiple_of(place_ref[2 * rank] * text_len, text_len), text_len)

    copies = []
    if last:
        out_hbm, out_ref, sems = refs[-3:]
        for k, (ref, (place, lane)) in enumerate(zip(refs[:-3], places)):
            there = out_hbm.at[rows_of(place), pl.ds(lane, ref.shape[1])]
            copies.append(pltpu.make_async_copy(ref, there, sems.at[k]))
    else:
        (out_ref,) = refs
    for copy in copies:
        copy.start()
    images = place_ref[2 * rank + 1]
    keep = lax.broadcasted_iota(jnp.int32, (token_count, HD), 0) < images * PATCH
    zero = jnp.zeros((token_count, HD), jnp.float32)
    ones = jnp.where(keep, zero + 1.0, zero).astype(jnp.bfloat16)
    queries_at = rows_of(rank)
    stack = 2 if unrolled and group % 2 == 0 else 4 if group % 4 == 0 else 1
    steps = group // stack
    wide = stack * HD

    def step(i, carry):
        column = i // steps * (2 * HD)
        at = i * wide
        if not unrolled:
            column = pl.multiple_of(lax.div(i, jnp.int32(steps)) * (2 * HD), 2 * HD)
            at = pl.multiple_of(at, wide)
        key = kv_ref[:, pl.ds(column, HD)]
        value = jnp.where(
            keep, kv_ref[:, pl.ds(column + HD, HD)].astype(jnp.float32), zero
        ).astype(jnp.bfloat16)
        queries = query_ref[queries_at, pl.ds(start + at, wide)]
        scores = lax.dot_general(
            jnp.concatenate([queries[:, k * HD : (k + 1) * HD] for k in range(stack)], axis=0),
            key,
            (((1,), (1,)), ((), ())),
            preferred_element_type=jnp.float32,
        )
        exponent = jnp.exp(scores).astype(jnp.bfloat16)
        summed = jnp.dot(
            exponent, jnp.concatenate([value, ones], axis=1), preferred_element_type=jnp.float32
        )
        context = (summed[:, :HD] / summed[:, HD:]).astype(jnp.bfloat16)
        out_ref[:, pl.ds(at, wide)] = jnp.concatenate(
            [context[k * text_len : (k + 1) * text_len] for k in range(stack)], axis=1
        )
        return carry

    if unrolled:
        for i in range(cols // wide):
            step(i, 0)
    else:
        lax.fori_loop(0, cols // wide, step, 0)
    if last:
        there = out_hbm.at[rows_of(rank), pl.ds(start, cols)]
        copies.append(pltpu.make_async_copy(out_ref, there, sems.at[len(places)]))
        copies[-1].start()
    for copy in copies:
        copy.wait()


def attend(place, query_normed, kv, first, pieces, last, unrolled, rank, samples_here, group):
    rows, cols = query_normed.shape
    token_count, kv_cols = kv.shape
    text_len = rows // samples_here
    heads = kv_cols // (2 * HD) * group
    pieces = pieces if last else []
    smem = pl.BlockSpec(memory_space=pltpu.SMEM)
    vmem = pl.BlockSpec(memory_space=pltpu.VMEM)
    return pl.pallas_call(
        functools.partial(
            attend_body,
            rank,
            samples_here,
            group,
            first,
            last,
            unrolled,
            [piece[1:] for piece in pieces],
        ),
        in_specs=[smem, vmem, vmem] + [vmem] * len(pieces),
        out_specs=pl.BlockSpec(memory_space=pltpu.HBM) if last else vmem,
        out_shape=pltpu.HBM((rows, cols), jnp.bfloat16)
        if last
        else jax.ShapeDtypeStruct((text_len, heads * HD), jnp.bfloat16),
        scratch_shapes=[
            pltpu.VMEM((text_len, heads * HD), jnp.bfloat16),
            pltpu.SemaphoreType.DMA((len(pieces) + 1,)),
        ]
        * last,
        cost_estimate=pl.CostEstimate(
            flops=6 * heads * text_len * token_count * HD,
            bytes_accessed=4 * text_len * heads * HD + 2 * token_count * kv_cols,
            transcendentals=heads * text_len * token_count,
        ),
        compiler_params=pltpu.CompilerParams(vmem_limit_bytes=24 << 20),
        name="attend",
    )(place, query_normed, kv, *[piece[0] for piece in pieces])


def moved(values, by):
    length = lax.axis_size("dp")
    if by % length == 0:
        return list(values)
    pairs = [(i, (i + by) % length) for i in range(length)]
    return [lax.ppermute(value, "dp", pairs) for value in values]


def by_shift(shift, start, finish):
    length = lax.axis_size("dp")
    digits = []
    unit = 1
    while unit < length:
        digits.append((unit, min(DIGIT, -(-length // unit))))
        unit *= digits[-1][1]
    if not digits:
        return finish(start(), lambda value: value, True)

    def choose(unit, choices, work):
        digit = shift
        if unit > 1:
            digit = lax.div(digit, jnp.int32(unit))
        if unit * choices < length:
            digit = lax.rem(digit, jnp.int32(choices))
        return conditionals._switch_internal(
            digit,
            [functools.partial(work, unit * k) for k in range(choices)],
            (),
            branches_platforms=None,
        )

    state = None
    for unit, choices in digits[:-1]:
        held = state

        def work(by):
            return moved(start() if held is None else held, by)

        state = choose(unit, choices, work)
    held = state

    def work(by):
        value = start() if held is None else held
        return finish(value, lambda value: moved(value, by), by == 0)

    return choose(*digits[-1], work)


def shards(queries, features, kv_weight, q_gain, k_gain, counts, owner):
    samples_here, token_count, _ = features.shape
    tensor_count = lax.axis_size("tensor")
    local_width = kv_weight.shape[1] // tensor_count
    repeats = max(1, 2 * HD // local_width)
    head_cols = local_width * repeats
    group = queries.shape[1] // HD // (head_cols // (2 * HD))
    k_gain = k_gain.reshape(1, HD)
    q_gain = q_gain.reshape(1, HD)

    def partials(wanted, width, after=(), counts=None, slots=None):
        return project(
            owner, features, kv_weight, wanted, head_cols, width, repeats, after, counts, slots
        )

    def swapped(part, bits):
        return lax.ppermute(part, "tensor", [(i, i ^ bits) for i in range(tensor_count)])

    def attention(rank, kv, pieces, unrolled):
        mine = []
        head = 0
        for k, part in enumerate(kv):
            last = rank == samples_here - 1 and k == len(kv) - 1
            out = attend(
                place,
                query_normed,
                part,
                head,
                pieces + mine,
                last,
                unrolled,
                rank,
                samples_here,
                group,
            )
            mine.append((out, rank, head * group * HD))
            head += part.shape[1] // (2 * HD)
        return out if last else mine

    ranks = range(samples_here)
    if tensor_count == 4 and head_cols == 4 * HD:
        def sent_of(rank):
            return [(rank, ((1, 0), (3, 0))), (rank, ((2, 1), (3, 1)))]

        def kept_of(rank):
            return [(rank, ((0, 0), (2, 0))), (rank, ((0, 1), (1, 1)))]

        *lead, slots = partials(sent_of(0), 2 * HD)
        sent = {0: lead}

        def first(rank):
            return [swapped(part, 1 + k) for k, part in enumerate(sent[rank])]

        def second(rank, got):
            added = add_halves(list(zip(kept[rank], got)))
            return [swapped(part, 2 - k) for k, part in enumerate(added)]

        def settled(rank, got, then):
            return combine(k_gain, list(zip(kept[rank], got, then)), 2 if rank > 0 else 1)

        got = first(0)
        early = [w for rank in ranks for w in kept_of(rank)]
        wanted = early + [sent_of(rank)[0] for rank in ranks[1:]]
        *planned, place = partials(wanted, 2 * HD, (), counts, slots)
        results = planned[:-samples_here]
        kept = {rank: results[2 * rank : 2 * rank + 2] for rank in ranks}
        sent.update({rank: [results[2 * samples_here - 1 + rank]] for rank in ranks[1:]})
        added = add_halves(list(zip(kept[0], got)))
        then = [swapped(part, 2 - k) for k, part in enumerate(added)]
        wanted = [sent_of(rank)[1] for rank in ranks[1:]]
        results = partials(wanted, 2 * HD, added[:1], None, slots)
        for rank in ranks[1:]:
            sent[rank].append(results[rank - 1])
    else:
        blocks = list(range(tensor_count - 1, -1, -1))
        heads = range(head_cols // (2 * HD))
        sent = {}
        slots = None
        for rank in ranks:
            known = counts if rank == samples_here - 1 and rank > 0 else None
            wanted = [(rank, ((block, head),)) for block in blocks for head in heads]
            results = partials(wanted, 2 * HD, (), known, slots)
            slots = results[-1] if rank == 0 else slots
            sent[rank] = results[: len(wanted)]
        *planned, place = results

        def first(rank):
            count = len(sent[rank]) - len(heads)
            return [swapped(part, blocks[k // len(heads)]) for k, part in enumerate(sent[rank][:count])]

        def second(rank, got):
            return []

        def settled(rank, got, then):
            mine = sent[rank][-len(heads) :]
            return combine(k_gain, [[mine[h]] + got[h :: len(heads)] for h in heads])

        got = first(0)
        then = []

    shifts = [shift.reshape(()) for shift in planned[-samples_here:]]
    kv = ready = query_normed = None
    pieces = []
    for rank in ranks:
        held, done, known = kv, list(pieces), ready
        last = rank == samples_here - 1

        def start():
            return list(settled(0, got, then)) if known is None else known

        def finish(value, move, still):
            if not last:
                coming = first(rank + 1)
            value = move(value)
            normed, more = None, []
            if rank == 0:
                normed = prepare(q_gain, queries)
            else:
                more = attention(rank - 1, held, [], still)
            if last:
                return attention(rank, value, done + more, True)
            following = list(settled(rank + 1, coming, second(rank + 1, coming)))
            return value, following, normed, [piece[0] for piece in more]

        moving = by_shift(shifts[rank], start, finish)
        if last:
            return moving
        before = [sum(part.shape[1] for part in kv[:k]) // (2 * HD) * group * HD for k in range(len(kv or []))]
        pieces += [(array, rank - 1, lane) for array, lane in zip(moving[3], before)]
        kv, ready = moving[:2]
        if rank == 0:
            query_normed = moving[2]


def solution(mesh):
    placed = (P("dp", "tensor"), P("dp", None, "tensor"), P("tensor", None), P(), P(), P(), P())
    return jax.shard_map(
        shards, mesh=mesh, in_specs=placed, out_specs=P("dp", "tensor"), check_vma=False
    )
```

```python
import functools
import math

import jax
import jax.numpy as jnp
from jax import lax
from jax._src.lax.control_flow import conditionals
from jax.experimental import pallas as pl
from jax.experimental.pallas import tpu as pltpu
from jax.sharding import PartitionSpec as P

HD = 128
PATCH = 24
EPS = 1e-05
DIGIT = 8


def ranked_slot(rank, owner_ref, samples_here, dp_count):
    if samples_here != 2:
        return rank
    reach = []
    for j in range(2):
        shift = lax.div(owner_ref[j], jnp.int32(2))
        reach.append(jnp.minimum(shift, dp_count - shift))
    return jnp.where(reach[1] > reach[0], 1 - rank, rank)


def project_body(samples_here, dp_count, repeats, wanted, head_cols, waits, splits, plan, leads, owner_ref, feature_hbm, weight_hbm, *rest):
    rest = rest[waits:]
    if plan:
        slots_ref, owner_ref, counts_ref, *rest = owner_ref, *rest
        slot_of = lambda rank: slots_ref[rank]
    elif leads:
        owner_hbm = owner_ref
        *rest, owner_ref, owner_sem = rest
        slot_of = lambda rank: ranked_slot(rank, owner_ref, samples_here, dp_count)
    else:
        slots_ref = owner_ref
        slot_of = lambda rank: slots_ref[rank]
    out_refs = rest[: len(wanted)]
    features, weights, feature_sem, weight_sem = rest[-4:]
    if plan:
        *shift_refs, place_ref = rest[len(wanted) : -4]
        for rank, shift_ref in enumerate(shift_refs):
            slot = slot_of(rank)
            shift = lax.div(owner_ref[slot], jnp.int32(samples_here))
            source = lax.axis_index("dp").astype(jnp.int32) - shift
            source = jnp.where(source < 0, source + dp_count, source)
            shift_ref[0] = shift
            place_ref[2 * rank] = slot
            place_ref[2 * rank + 1] = counts_ref[source * samples_here + slot]
    me = lax.axis_index("tensor").astype(jnp.int32)
    ranks = list(dict.fromkeys(rank for rank, _ in wanted))
    rows = list(dict.fromkeys(row for _, row in wanted))
    panels = [panel for row in rows for panel in row]
    width = weights.shape[2]
    token_count, depth = features.shape[1:]
    split = token_count // splits

    def feature_copy(k, part):
        at = pl.ds(part * split, split)
        return pltpu.make_async_copy(
            feature_hbm.at[slot_of(ranks[k]), at], features.at[k, at], feature_sem.at[k, part]
        )

    def weight_copy(k):
        block, piece = panels[k]
        head = lax.div(jnp.bitwise_xor(me, block), jnp.int32(repeats))
        start = pl.multiple_of(head * head_cols + piece * width, width)
        return pltpu.make_async_copy(
            weight_hbm.at[:, pl.ds(start, width)], weights.at[k], weight_sem.at[k]
        )

    weight_copies = [weight_copy(k) for k in range(len(panels))]
    ahead = 2
    if leads:
        owner_copy = pltpu.make_async_copy(owner_hbm, owner_ref, owner_sem)
        owner_copy.start()
    for copy in weight_copies[:ahead]:
        copy.start()
    if leads:
        owner_copy.wait()
        for rank in range(samples_here):
            rest[len(wanted)][rank] = slot_of(rank)
    feature_copies = [
        [feature_copy(k, part) for part in range(splits)] for k in range(len(ranks))
    ]
    for copy in feature_copies[0]:
        copy.start()
    for copies in feature_copies[1:]:
        for copy in copies:
            copy.start()
    for copies in feature_copies:
        for copy in copies:
            copy.wait()
    for copy in weight_copies[ahead:]:
        copy.start()
    base = 0
    for row in rows:
        takers = [(ref, ranks.index(rank)) for ref, (rank, taken) in zip(out_refs, wanted) if taken == row]
        joint = len(takers) > 1 and [r for _, r in takers] == list(range(len(ranks)))

        def step(p, carry, takers=takers, joint=joint, base=base):
            k = base + p
            pltpu.make_async_copy(
                weight_hbm.at[:, pl.ds(0, width)], weights.at[k], weight_sem.at[k]
            ).wait()
            lanes = pl.ds(pl.multiple_of(p * width, width), width)
            lefts = [features[...].reshape(-1, depth)] if joint else [features[r] for _, r in takers]
            products = [
                jnp.dot(left, weights[k], preferred_element_type=jnp.float32).astype(jnp.bfloat16)
                for left in lefts
            ]
            for at, (out_ref, _) in enumerate(takers):
                if joint:
                    out_ref[:, lanes] = products[0][at * token_count : (at + 1) * token_count]
                else:
                    out_ref[:, lanes] = products[at]
            return carry

        lax.fori_loop(0, len(row), step, 0)
        base += len(row)


def project(owner, features, kv_weight, wanted, head_cols, width, repeats, after=(), counts=None, slots=None):
    plan = counts is not None
    leads = slots is None
    samples_here, token_count, depth = features.shape
    ranks = len({rank for rank, _ in wanted})
    panels = len({panel for _, row in wanted for panel in row})
    work = sum(len(row) for _, row in wanted)
    splits = 2
    hbm = pl.BlockSpec(memory_space=pltpu.HBM)
    return pl.pallas_call(
        functools.partial(
            project_body,
            samples_here,
            lax.axis_size("dp"),
            repeats,
            wanted,
            head_cols,
            len(after),
            splits,
            plan,
            leads,
        ),
        in_specs=[hbm if leads else pl.BlockSpec(memory_space=pltpu.SMEM), hbm, hbm]
        + [pl.BlockSpec(memory_space=pl.ANY)] * len(after)
        + [pl.BlockSpec(memory_space=pltpu.SMEM)] * (2 * plan),
        out_specs=[pl.BlockSpec(memory_space=pltpu.VMEM)] * len(wanted)
        + [pl.BlockSpec(memory_space=pltpu.SMEM)] * ((samples_here + 1) * plan + leads),
        out_shape=[
            pltpu.VMEM((token_count, width * len(row)), jnp.bfloat16) for _, row in wanted
        ]
        + [pltpu.SMEM((1,), jnp.int32)] * (samples_here * plan)
        + [pltpu.SMEM((2 * samples_here,), jnp.int32)] * plan
        + [pltpu.SMEM((samples_here,), jnp.int32)] * leads,
        scratch_shapes=[
            pltpu.VMEM((ranks, token_count, depth), jnp.bfloat16),
            pltpu.VMEM((panels, depth, width), jnp.bfloat16),
            pltpu.SemaphoreType.DMA((ranks, splits)),
            pltpu.SemaphoreType.DMA((panels,)),
        ]
        + [pltpu.SMEM(owner.shape, jnp.int32), pltpu.SemaphoreType.DMA] * leads,
        cost_estimate=pl.CostEstimate(
            flops=2 * work * token_count * depth * width,
            bytes_accessed=2 * (token_count * ranks + width * panels) * depth,
            transcendentals=0,
        ),
        compiler_params=pltpu.CompilerParams(vmem_limit_bytes=58 << 20),
        name="project",
    )(owner if leads else slots, features, kv_weight, *after, *([owner, counts] * plan))


def mean_square(value):
    square = value * value
    high = square.astype(jnp.bfloat16)
    low = (square - high.astype(jnp.float32)).astype(jnp.bfloat16)
    parts = jnp.concatenate([high, low], axis=1)
    ones = jnp.ones((2 * HD, HD), jnp.bfloat16)
    return jnp.dot(parts, ones, preferred_element_type=jnp.float32) * (1.0 / HD)


def add_body(*refs):
    count = len(refs) // 3
    for k in range(count):
        ref, other, out_ref = refs[2 * k], refs[2 * k + 1], refs[2 * count + k]
        cols = out_ref.shape[1]
        out_ref[...] = (
            ref[:, cols:].astype(jnp.float32) + other[:, cols:].astype(jnp.float32)
        ).astype(jnp.bfloat16)


def add_halves(pairs):
    vmem = pl.BlockSpec(memory_space=pltpu.VMEM)
    shapes = [jax.ShapeDtypeStruct((p.shape[0], p.shape[1] // 2), p.dtype) for p, _ in pairs]
    return pl.pallas_call(
        add_body,
        in_specs=[vmem] * (2 * len(pairs)),
        out_specs=[vmem] * len(pairs),
        out_shape=shapes,
        cost_estimate=pl.CostEstimate(
            flops=sum(shape.size for shape in shapes),
            bytes_accessed=6 * sum(shape.size for shape in shapes),
            transcendentals=0,
        ),
        compiler_params=pltpu.CompilerParams(vmem_limit_bytes=16 << 20),
        name="add_halves",
    )(*[part for pair in pairs for part in pair])


def combine_body(layout, gain_ref, *refs):
    out_refs = refs[sum(layout) :]
    gain = gain_ref[...]
    at = 0
    for head, count in enumerate(layout):
        part_refs = refs[at : at + count]
        at += count
        each = len(layout) // len(out_refs)
        out_ref = out_refs[head // each]
        rows = out_ref.shape[0]
        tile = 192 if rows % 192 == 0 else rows

        def step(i, carry):
            here = pl.ds(pl.multiple_of(i * tile, tile), tile)
            for column in (0, HD):
                lanes = slice(column, column + HD)
                total = part_refs[0][here, lanes].astype(jnp.float32)
                for ref in part_refs[1:]:
                    total = total + ref[here, lanes].astype(jnp.float32)
                if column == 0:
                    total = total * lax.rsqrt(mean_square(total) + EPS) * gain
                start = 2 * HD * (head % each) + column
                lanes = slice(start, start + HD)
                out_ref[here, lanes] = total.astype(jnp.bfloat16)
            return carry

        lax.fori_loop(0, rows // tile, step, 0)


def combine(k_gain, heads, outputs=1):
    rows = heads[0][0].shape[0]
    parts = [part for head in heads for part in head]
    vmem = pl.BlockSpec(memory_space=pltpu.VMEM)
    return pl.pallas_call(
        functools.partial(combine_body, [len(head) for head in heads]),
        in_specs=[vmem] * (len(parts) + 1),
        out_specs=[vmem] * outputs,
        out_shape=[jax.ShapeDtypeStruct((rows, 2 * HD * len(heads) // outputs), jnp.bfloat16)]
        * outputs,
        cost_estimate=pl.CostEstimate(
            flops=2 * rows * HD * (len(parts) + 4),
            bytes_accessed=4 * rows * HD * (len(parts) + len(heads)),
            transcendentals=rows * len(heads),
        ),
        compiler_params=pltpu.CompilerParams(vmem_limit_bytes=16 << 20),
        name="combine",
    )(k_gain, *parts)


def prepare_body(gain_ref, query_ref, out_ref):
    gain = gain_ref[...] * (1.0 / math.sqrt(HD))
    rows, cols = query_ref.shape
    tile = 224 if rows % 224 == 0 else rows

    def step(i, carry):
        here = pl.ds(pl.multiple_of(i * tile, tile), tile)
        for column in range(0, cols, HD):
            head = query_ref[here, column : column + HD].astype(jnp.float32)
            out_ref[here, column : column + HD] = (
                head * lax.rsqrt(mean_square(head) + EPS) * gain
            ).astype(jnp.bfloat16)
        return carry

    lax.fori_loop(0, rows // tile, step, 0)


def prepare(q_gain, queries):
    rows, cols = queries.shape
    tile = cols // 8 if cols % (8 * HD) == 0 else cols
    block = pl.BlockSpec((rows, tile), lambda i: (0, i))
    return pl.pallas_call(
        prepare_body,
        grid=(cols // tile,),
        in_specs=[pl.BlockSpec((1, HD), lambda i: (0, 0)), block],
        out_specs=block,
        out_shape=jax.ShapeDtypeStruct((rows, cols), jnp.bfloat16),
        cost_estimate=pl.CostEstimate(
            flops=rows * cols * 6, bytes_accessed=4 * rows * cols, transcendentals=rows * cols // HD
        ),
        compiler_params=pltpu.CompilerParams(vmem_limit_bytes=24 << 20),
        name="prepare",
    )(q_gain, queries)


def attend_body(rank, samples_here, group, first, last, unrolled, places, place_ref, query_ref, kv_ref, *refs):
    token_count, kv_cols = kv_ref.shape
    text_len = query_ref.shape[0] // samples_here
    cols = kv_cols // (2 * HD) * group * HD
    start = first * group * HD

    def rows_of(rank):
        return pl.ds(pl.multiple_of(place_ref[2 * rank] * text_len, text_len), text_len)

    copies = []
    if last:
        out_hbm, out_ref, sems = refs[-3:]
        for k, (ref, (place, lane)) in enumerate(zip(refs[:-3], places)):
            there = out_hbm.at[rows_of(place), pl.ds(lane, ref.shape[1])]
            copies.append(pltpu.make_async_copy(ref, there, sems.at[k]))
    else:
        (out_ref,) = refs
    for copy in copies:
        copy.start()
    images = place_ref[2 * rank + 1]
    keep = lax.broadcasted_iota(jnp.int32, (token_count, HD), 0) < images * PATCH
    zero = jnp.zeros((token_count, HD), jnp.float32)
    ones = jnp.where(keep, zero + 1.0, zero).astype(jnp.bfloat16)
    queries_at = rows_of(rank)
    stack = 2 if unrolled and group % 2 == 0 else 4 if group % 4 == 0 else 1
    steps = group // stack
    wide = stack * HD

    def step(i, carry):
        column = i // steps * (2 * HD)
        at = i * wide
        if not unrolled:
            column = pl.multiple_of(lax.div(i, jnp.int32(steps)) * (2 * HD), 2 * HD)
            at = pl.multiple_of(at, wide)
        key = kv_ref[:, pl.ds(column, HD)]
        value = jnp.where(
            keep, kv_ref[:, pl.ds(column + HD, HD)].astype(jnp.float32), zero
        ).astype(jnp.bfloat16)
        queries = query_ref[queries_at, pl.ds(start + at, wide)]
        scores = lax.dot_general(
            jnp.concatenate([queries[:, k * HD : (k + 1) * HD] for k in range(stack)], axis=0),
            key,
            (((1,), (1,)), ((), ())),
            preferred_element_type=jnp.float32,
        )
        exponent = jnp.exp(scores).astype(jnp.bfloat16)
        summed = jnp.dot(
            exponent, jnp.concatenate([value, ones], axis=1), preferred_element_type=jnp.float32
        )
        context = (summed[:, :HD] / summed[:, HD:]).astype(jnp.bfloat16)
        out_ref[:, pl.ds(at, wide)] = jnp.concatenate(
            [context[k * text_len : (k + 1) * text_len] for k in range(stack)], axis=1
        )
        return carry

    if unrolled:
        for i in range(cols // wide):
            step(i, 0)
    else:
        lax.fori_loop(0, cols // wide, step, 0)
    if last:
        there = out_hbm.at[rows_of(rank), pl.ds(start, cols)]
        copies.append(pltpu.make_async_copy(out_ref, there, sems.at[len(places)]))
        copies[-1].start()
    for copy in copies:
        copy.wait()


def attend(place, query_normed, kv, first, pieces, last, unrolled, rank, samples_here, group):
    rows, cols = query_normed.shape
    token_count, kv_cols = kv.shape
    text_len = rows // samples_here
    heads = kv_cols // (2 * HD) * group
    pieces = pieces if last else []
    smem = pl.BlockSpec(memory_space=pltpu.SMEM)
    vmem = pl.BlockSpec(memory_space=pltpu.VMEM)
    return pl.pallas_call(
        functools.partial(
            attend_body,
            rank,
            samples_here,
            group,
            first,
            last,
            unrolled,
            [piece[1:] for piece in pieces],
        ),
        in_specs=[smem, vmem, vmem] + [vmem] * len(pieces),
        out_specs=pl.BlockSpec(memory_space=pltpu.HBM) if last else vmem,
        out_shape=pltpu.HBM((rows, cols), jnp.bfloat16)
        if last
        else jax.ShapeDtypeStruct((text_len, heads * HD), jnp.bfloat16),
        scratch_shapes=[
            pltpu.VMEM((text_len, heads * HD), jnp.bfloat16),
            pltpu.SemaphoreType.DMA((len(pieces) + 1,)),
        ]
        * last,
        cost_estimate=pl.CostEstimate(
            flops=6 * heads * text_len * token_count * HD,
            bytes_accessed=4 * text_len * heads * HD + 2 * token_count * kv_cols,
            transcendentals=heads * text_len * token_count,
        ),
        compiler_params=pltpu.CompilerParams(vmem_limit_bytes=24 << 20),
        name="attend",
    )(place, query_normed, kv, *[piece[0] for piece in pieces])


def moved(values, by):
    length = lax.axis_size("dp")
    if by % length == 0:
        return list(values)
    pairs = [(i, (i + by) % length) for i in range(length)]
    return [lax.ppermute(value, "dp", pairs) for value in values]


def by_shift(shift, start, finish):
    length = lax.axis_size("dp")
    digits = []
    unit = 1
    while unit < length:
        digits.append((unit, min(DIGIT, -(-length // unit))))
        unit *= digits[-1][1]
    if not digits:
        return finish(start(), lambda value: value, True)

    def choose(unit, choices, work):
        digit = shift
        if unit > 1:
            digit = lax.div(digit, jnp.int32(unit))
        if unit * choices < length:
            digit = lax.rem(digit, jnp.int32(choices))
        return conditionals._switch_internal(
            digit,
            [functools.partial(work, unit * k) for k in range(choices)],
            (),
            branches_platforms=None,
        )

    state = None
    for unit, choices in digits[:-1]:
        held = state

        def work(by):
            return moved(start() if held is None else held, by)

        state = choose(unit, choices, work)
    held = state

    def work(by):
        value = start() if held is None else held
        return finish(value, lambda value: moved(value, by), by == 0)

    return choose(*digits[-1], work)


def shards(queries, features, kv_weight, q_gain, k_gain, counts, owner):
    samples_here, token_count, _ = features.shape
    tensor_count = lax.axis_size("tensor")
    local_width = kv_weight.shape[1] // tensor_count
    repeats = max(1, 2 * HD // local_width)
    head_cols = local_width * repeats
    group = queries.shape[1] // HD // (head_cols // (2 * HD))
    k_gain = k_gain.reshape(1, HD)
    q_gain = q_gain.reshape(1, HD)

    def partials(wanted, width, after=(), counts=None, slots=None):
        return project(
            owner, features, kv_weight, wanted, head_cols, width, repeats, after, counts, slots
        )

    def swapped(part, bits):
        return lax.ppermute(part, "tensor", [(i, i ^ bits) for i in range(tensor_count)])

    def attention(rank, kv, pieces, unrolled):
        mine = []
        head = 0
        for k, part in enumerate(kv):
            last = rank == samples_here - 1 and k == len(kv) - 1
            out = attend(
                place,
                query_normed,
                part,
                head,
                pieces + mine,
                last,
                unrolled,
                rank,
                samples_here,
                group,
            )
            mine.append((out, rank, head * group * HD))
            head += part.shape[1] // (2 * HD)
        return out if last else mine

    ranks = range(samples_here)
    if tensor_count == 4 and head_cols == 4 * HD:
        def sent_of(rank):
            return [(rank, ((1, 0), (3, 0))), (rank, ((2, 1), (3, 1)))]

        def kept_of(rank):
            return [(rank, ((0, 0), (2, 0))), (rank, ((0, 1), (1, 1)))]

        *lead, slots = partials(sent_of(0), 2 * HD)
        sent = {0: lead}

        def first(rank):
            return [swapped(part, 1 + k) for k, part in enumerate(sent[rank])]

        def second(rank, got):
            added = add_halves(list(zip(kept[rank], got)))
            return [swapped(part, 2 - k) for k, part in enumerate(added)]

        def settled(rank, got, then):
            return combine(k_gain, list(zip(kept[rank], got, then)), 2 if rank > 0 else 1)

        got = first(0)
        early = [w for rank in ranks for w in kept_of(rank)]
        wanted = early + [sent_of(rank)[0] for rank in ranks[1:]]
        *planned, place = partials(wanted, 2 * HD, (), counts, slots)
        results = planned[:-samples_here]
        kept = {rank: results[2 * rank : 2 * rank + 2] for rank in ranks}
        sent.update({rank: [results[2 * samples_here - 1 + rank]] for rank in ranks[1:]})
        added = add_halves(list(zip(kept[0], got)))
        then = [swapped(part, 2 - k) for k, part in enumerate(added)]
        wanted = [sent_of(rank)[1] for rank in ranks[1:]]
        results = partials(wanted, 2 * HD, added[:1], None, slots)
        for rank in ranks[1:]:
            sent[rank].append(results[rank - 1])
    else:
        blocks = list(range(tensor_count - 1, -1, -1))
        heads = range(head_cols // (2 * HD))
        sent = {}
        slots = None
        for rank in ranks:
            known = counts if rank == samples_here - 1 and rank > 0 else None
            wanted = [(rank, ((block, head),)) for block in blocks for head in heads]
            results = partials(wanted, 2 * HD, (), known, slots)
            slots = results[-1] if rank == 0 else slots
            sent[rank] = results[: len(wanted)]
        *planned, place = results

        def first(rank):
            count = len(sent[rank]) - len(heads)
            return [swapped(part, blocks[k // len(heads)]) for k, part in enumerate(sent[rank][:count])]

        def second(rank, got):
            return []

        def settled(rank, got, then):
            mine = sent[rank][-len(heads) :]
            return combine(k_gain, [[mine[h]] + got[h :: len(heads)] for h in heads])

        got = first(0)
        then = []

    shifts = [shift.reshape(()) for shift in planned[-samples_here:]]
    kv = ready = query_normed = None
    pieces = []
    for rank in ranks:
        held, done, known = kv, list(pieces), ready
        last = rank == samples_here - 1

        def start():
            return list(settled(0, got, then)) if known is None else known

        def finish(value, move, still):
            if not last:
                coming = first(rank + 1)
            value = move(value)
            normed, more = None, []
            if rank == 0:
                normed = prepare(q_gain, queries)
            else:
                more = attention(rank - 1, held, [], still)
            if last:
                return attention(rank, value, done + more, True)
            following = list(settled(rank + 1, coming, second(rank + 1, coming)))
            return value, following, normed, [piece[0] for piece in more]

        moving = by_shift(shifts[rank], start, finish)
        if last:
            return moving
        before = [sum(part.shape[1] for part in kv[:k]) // (2 * HD) * group * HD for k in range(len(kv or []))]
        pieces += [(array, rank - 1, lane) for array, lane in zip(moving[3], before)]
        kv, ready = moving[:2]
        if rank == 0:
            query_normed = moving[2]


def solution(mesh):
    placed = (P("dp", "tensor"), P("dp", None, "tensor"), P("tensor", None), P(), P(), P(), P())
    return jax.shard_map(
        shards, mesh=mesh, in_specs=placed, out_specs=P("dp", "tensor"), check_vma=False
    )
```
